256 devices in a mesh: grp: 4 (over z_lo, core), sub: 64 (over x, z_hi, y).
Axes of the slice: x: 4, y: 4, z: 8 (z_hi: 4, z_lo: 2; z = z_hi * 2 + z_lo), core: 2. Of those that a mesh axis runs over, the one named last changes fastest.
Arguments:
- snapshots: bfloat16 [2048, 2, 256, 128], P(None, None, ('grp', 'sub')), may hold values from -6 to 6
- steering: bfloat16 [256, 2, 128, 64], P(('grp', 'sub')), may hold values from -0.375 to 0.375
- combining: bfloat16 [256, 2, 64, 1024], P(('grp', 'sub')), may hold values from -0.03125 to 0.03125
- beam_list: int32 [1024], replicated, may hold values from 0 to 1023, each once
Outputs:
- beams_out: bfloat16 [2, 2048, 1024], P(None, ('grp', 'sub'))
The draws below stay inside these ranges and needn't reach their ends.
Inputs may be any that keep to these rules, and one draw needn't show every extreme that they name: `beam_list`: each of the 1024 beams appears once.
All inputs are finite; a program needn't handle non-finite values.
Results may differ from the reference program's by a relative error of at most 0.0065.
Values may be sent and summed in bfloat16 or wider, within the bound.
A program may use at most 128 MiB of HBM per device.

```python
import jax
import jax.numpy as jnp
from jax import lax

EL = 128
PB = 64
NBEAM = 1024
SNAP = 2048
SUBS = 256


def level_of(stream_key, extent, pieces, smallest, largest):
    def one(dim, blocks):
        draws = jax.random.uniform(jax.random.fold_in(jax.random.fold_in(stream_key, 6), dim), (blocks,), jnp.float32, smallest / len(pieces), largest / len(pieces))
        return jnp.repeat(jnp.exp(draws), extent[dim] // blocks).reshape((-1,) + (1,) * (len(extent) - dim - 1))

    factor_of = one(*pieces[0])
    for cut in pieces[1:]:
        factor_of = factor_of * one(*cut)
    return factor_of


def noise(rng, dims, width, limit, shards=(), kind=jnp.bfloat16):
    result = jax.random.normal(rng, dims, jnp.float32) * width
    if len(shards) > 0:
        result = level_of(rng, dims, shards, -0.22, 0.18) * result
    return jnp.clip(result, min=-limit, max=limit).astype(kind)


def setup_inputs(seed: int = 0) -> dict:
    keys = jax.random.split(jax.random.key(seed), 5)
    return {
        "snapshots": noise(keys[0], (SNAP, 2, SUBS, EL), 1.0, 6.0, ((2, 256),)),
        "steering": noise(keys[1], (SUBS, 2, EL, PB), (2 * EL) ** -0.5, 0.375, ((0, 256),)),
        "combining": noise(keys[2], (SUBS, 2, PB, NBEAM), (2 * SUBS * PB) ** -0.5, 0.03125, ((0, 256),)),
        "beam_list": jax.random.permutation(keys[3], NBEAM).astype(jnp.int32),
    }


def reference(snapshots, steering, combining, beam_list):
    ordered = jnp.take(combining, beam_list, axis=3)

    def accumulate(subarray, running):
        signal = lax.dynamic_index_in_dim(snapshots, subarray, 2, keepdims=False).astype(jnp.float32)
        steer_s = lax.dynamic_index_in_dim(steering, subarray, 0, keepdims=False).astype(jnp.float32)
        comb_s = lax.dynamic_index_in_dim(ordered, subarray, 0, keepdims=False).astype(jnp.float32)
        sig_real = signal[:, 0]
        sig_imag = signal[:, 1]
        beam_real = jnp.dot(sig_real, steer_s[0]) - jnp.dot(sig_imag, steer_s[1])
        beam_imag = jnp.dot(sig_real, steer_s[1]) + jnp.dot(sig_imag, steer_s[0])
        beam_real = lax.optimization_barrier(beam_real.astype(jnp.bfloat16)).astype(jnp.float32)
        beam_imag = lax.optimization_barrier(beam_imag.astype(jnp.bfloat16)).astype(jnp.float32)
        final_real = jnp.dot(beam_real, comb_s[0]) - jnp.dot(beam_imag, comb_s[1])
        final_imag = jnp.dot(beam_real, comb_s[1]) + jnp.dot(beam_imag, comb_s[0])
        return running + jnp.stack([final_real, final_imag])

    running = lax.fori_loop(0, SUBS, accumulate, jnp.zeros((2, SNAP, NBEAM), jnp.float32))
    return running.astype(jnp.bfloat16)
```

```python
import functools

import jax
import jax.numpy as jnp
from jax import lax
from jax.experimental import pallas as pl
from jax.experimental.pallas import tpu as pltpu
from jax.sharding import PartitionSpec as P

MESH = pl.DeviceIdType.MESH
NCH = 4
BF = jnp.bfloat16
F32 = jnp.float32


def kernel(
    snap_ref, steer_ref, comb_ref, list_ref, out_ref,
    snap, steer, prod, p_send, p_all, lhs, w_all, sel, part, relay, ysum, yfin, tsum, zrecv, acc,
    load_sem, wload_sem, p_ss, p_rs, w_ss, w_rs, y_ss, y_rs, z_ss, z_rs,
):
    width = w_all.shape[-1]
    grp = lax.axis_index("grp")
    sub = lax.axis_index("sub")
    zl, core = grp // 2, grp % 2
    x, zh, y = sub // 16, (sub // 4) % 4, sub % 4
    z = zh * 2 + zl
    xp, xm, xo = (x + 1) % 4, (x + 3) % 4, (x + 2) % 4
    yp, ym, yo = (y + 1) % 4, (y + 3) % 4, (y + 2) % 4
    me = x * 2 + core

    def dev_x(x2, c2):
        return (zl * 2 + c2, x2 * 16 + zh * 4 + y)

    def dev_y(y2):
        return (grp, x * 16 + zh * 4 + y2)

    def dev_z(z2):
        return ((z2 % 2) * 2 + core, x * 16 + (z2 // 2) * 4 + y)

    def zrow(z2):
        return (z2 % 2) * 4 + z2 // 2

    loads = [
        pltpu.make_async_copy(steer_ref, steer, load_sem.at[0]),
        pltpu.make_async_copy(snap_ref, snap, load_sem.at[1]),
    ]
    for c in loads:
        c.start()
    wloads = []
    for ch in range(NCH):
        c = pltpu.make_async_copy(
            comb_ref.at[:, :, pl.ds(ch * width, width)], w_all.at[ch, me], wload_sem.at[ch]
        )
        c.start()
        wloads.append(c)

    barrier = pltpu.get_barrier_semaphore()
    peers = [dev_x((x + dx) % 4, core if dc == 0 else 1 - core)
             for dx in range(4) for dc in range(2) if dx or dc]
    peers += [dev_y(yp), dev_y(ym)]
    peers += [dev_z((z + dz) % 8) for dz in range(1, 8)]
    for p in peers:
        pl.semaphore_signal(barrier, inc=1, device_id=p, device_id_type=MESH)

    sends = []

    def remote(src, dst, ss, rs, dev):
        return pltpu.make_async_remote_copy(
            src_ref=src, dst_ref=dst, send_sem=ss, recv_sem=rs, device_id=dev, device_id_type=MESH
        )

    def send(src, dst, ss, rs, dev):
        c = remote(src, dst, ss, rs, dev)
        c.start()
        sends.append(c)

    def arrived(dst, ss, rs, dev):
        remote(dst, dst, ss, rs, dev).wait_recv()

    for c in loads:
        c.wait()
    s_re, s_im = steer[0], steer[1]
    weights = jnp.concatenate([s_re, s_im, -s_im, s_re], axis=0)
    order = [(2, 0), (2, 1), (1, 0), (1, 1), (3, 0), (3, 1), (0, 1), (0, 0)]
    for n, (dx, dc) in enumerate(order):
        x2 = (x + dx) % 4
        c2 = core if dc == 0 else 1 - core
        dest = x2 * 2 + c2
        for half in range(2):
            block = half * 8 + c2 * 4 + x2
            rows = snap[pl.ds(pl.multiple_of(block * 256, 256), 256), :]
            slot = n * 2 + half
            both = lax.dot_general(
                rows, weights, (((1,), (1,)), ((), ())), preferred_element_type=F32
            )
            prod[slot, 0] = both[:, :128]
            prod[slot, 1] = both[:, 128:]
            val = prod[slot, 0, pl.ds(0, 128, stride=2)] + prod[slot, 1, pl.ds(1, 128, stride=2)]
            for q in range(4):
                got = jnp.concatenate(
                    [val[h * 32 + q * 8 : h * 32 + q * 8 + 8] for h in range(4)], axis=0
                )
                p_send[dest, q, pl.ds(half * 32, 32), :] = got.astype(BF)

    pl.semaphore_wait(barrier, len(peers))

    def w_own(ch):
        wloads[ch].wait()
        mine = w_all.at[ch, me]
        send(mine, mine, w_ss.at[ch, 0], w_rs.at[ch, 0], dev_x(xp, core))
        send(mine, mine, w_ss.at[ch, 1], w_rs.at[ch, 1], dev_x(xm, core))
        send(mine, mine, w_ss.at[ch, 4], w_rs.at[ch, 4], dev_x(x, 1 - core))

    def p_sends():
        for dx, dc in order[:-1]:
            x2 = (x + dx) % 4
            c2 = core if dc == 0 else 1 - core
            r = dx * 2 + dc
            send(p_send.at[x2 * 2 + c2], p_all.at[me], p_ss.at[r], p_rs.at[r], dev_x(x2, c2))

    def w_relay(ch):
        a = w_all.at[ch, xm * 2 + core]
        b = w_all.at[ch, xp * 2 + core]
        arrived(a, w_ss.at[ch, 0], w_rs.at[ch, 0], dev_x(xp, core))
        send(a.at[0], a.at[0], w_ss.at[ch, 2], w_rs.at[ch, 2], dev_x(xp, core))
        send(a, a, w_ss.at[ch, 5], w_rs.at[ch, 5], dev_x(x, 1 - core))
        arrived(b, w_ss.at[ch, 1], w_rs.at[ch, 1], dev_x(xm, core))
        send(b.at[1], b.at[1], w_ss.at[ch, 3], w_rs.at[ch, 3], dev_x(xm, core))
        send(b, b, w_ss.at[ch, 6], w_rs.at[ch, 6], dev_x(x, 1 - core))

    def w_finish(ch):
        o = w_all.at[ch, xo * 2 + core]
        arrived(o.at[0], w_ss.at[ch, 2], w_rs.at[ch, 2], dev_x(xp, core))
        arrived(o.at[1], w_ss.at[ch, 3], w_rs.at[ch, 3], dev_x(xm, core))
        send(o, o, w_ss.at[ch, 7], w_rs.at[ch, 7], dev_x(x, 1 - core))
        for role, x2 in ((4, x), (5, xm), (6, xp), (7, xo)):
            arrived(
                w_all.at[ch, x2 * 2 + 1 - core], w_ss.at[ch, role], w_rs.at[ch, role],
                dev_x(x, 1 - core),
            )

    def build_lhs():
        sign = jnp.where(lax.broadcasted_iota(jnp.int32, (256, 128), 1) < 64, 1.0, -1.0)
        for dx, dc in [(0, 0)] + order[:-1]:
            x2 = (x + 4 - dx) % 4
            c2 = core if dc == 0 else 1 - core
            src = x2 * 2 + c2
            if dx or dc:
                r = dx * 2 + dc
                arrived(p_all.at[src], p_ss.at[r], p_rs.at[r], dev_x(x2, c2))
                val = p_all[src]
            else:
                val = p_send[src]
            val = val.reshape(256, 128).astype(F32)
            top = (val * sign).reshape(32, 8, 128)
            low = pltpu.roll(val, 64, 1).reshape(32, 8, 128)
            lhs[src] = jnp.concatenate([top, low], axis=1).astype(BF).reshape(512, 128)

    def multiply(ch):
        left = jnp.concatenate([lhs[k] for k in range(8)], axis=1)
        right = w_all[ch].reshape(1024, width)
        val = jnp.dot(left, right, preferred_element_type=F32)
        part[ch] = val.astype(BF).reshape(4, 8, 16, width)

    lo, hi = pl.ds(0, 4), pl.ds(4, 4)

    def y_first(ch):
        send(part.at[ch, yo, lo], relay.at[ch, 0], y_ss.at[ch, 0], y_rs.at[ch, 0], dev_y(yp))
        send(part.at[ch, yo, hi], relay.at[ch, 1], y_ss.at[ch, 1], y_rs.at[ch, 1], dev_y(ym))
        send(part.at[ch, yp, hi], yfin.at[ch, 0, hi], y_ss.at[ch, 3], y_rs.at[ch, 3], dev_y(yp))
        send(part.at[ch, ym, lo], yfin.at[ch, 1, lo], y_ss.at[ch, 4], y_rs.at[ch, 4], dev_y(ym))

    def y_relay(ch):
        arrived(relay.at[ch, 0], y_ss.at[ch, 0], y_rs.at[ch, 0], dev_y(yp))
        ysum[ch, 0] = (part[ch, yp, lo].astype(F32) + relay[ch, 0].astype(F32)).astype(BF)
        arrived(relay.at[ch, 1], y_ss.at[ch, 1], y_rs.at[ch, 1], dev_y(ym))
        ysum[ch, 1] = (part[ch, ym, hi].astype(F32) + relay[ch, 1].astype(F32)).astype(BF)
        send(ysum.at[ch, 0], yfin.at[ch, 0, lo], y_ss.at[ch, 2], y_rs.at[ch, 2], dev_y(yp))
        send(ysum.at[ch, 1], yfin.at[ch, 1, hi], y_ss.at[ch, 5], y_rs.at[ch, 5], dev_y(ym))

    def y_finish(ch):
        for role, k, rows, y2 in ((3, 0, hi, yp), (4, 1, lo, ym), (2, 0, lo, yp), (5, 1, hi, ym)):
            arrived(yfin.at[ch, k, rows], y_ss.at[ch, role], y_rs.at[ch, role], dev_y(y2))
        total = part[ch, y].astype(F32) + yfin[ch, 0].astype(F32) + yfin[ch, 1].astype(F32)
        tsum[ch] = total.astype(BF)
        for dz in (4, 3, 5, 2, 6, 1, 7):
            z2 = (z + dz) % 8
            send(tsum.at[ch, zrow(z2)], zrecv.at[ch, dz], z_ss.at[ch, dz], z_rs.at[ch, dz], dev_z(z2))

    def z_finish(ch):
        total = tsum[ch, zrow(z)].astype(F32)
        for dz in range(1, 8):
            arrived(zrecv.at[ch, dz], z_ss.at[ch, dz], z_rs.at[ch, dz], dev_z((z + dz) % 8))
        for dz in range(1, 8):
            total = total + zrecv[ch, dz].astype(F32)
        val = jnp.dot(total.astype(BF), sel[ch], preferred_element_type=F32)
        if ch == 0:
            acc[...] = val
        elif ch < NCH - 1:
            acc[...] += val
        else:
            out_ref[...] = (acc[...] + val).astype(BF)

    w_own(0)
    p_sends()
    w_own(1)
    for ch in range(NCH):
        rows = lax.broadcasted_iota(jnp.int32, (width, 1024), 0) + ch * width
        sel[ch] = jnp.where(rows == list_ref[...], 1.0, 0.0).astype(BF)
    for step in range(NCH + 2):
        if step < NCH:
            w_relay(step)
            if step + 2 < NCH:
                w_own(step + 2)
            if step == 0:
                build_lhs()
        if 1 <= step <= NCH:
            y_relay(step - 1)
        if step < NCH:
            w_finish(step)
            multiply(step)
            y_first(step)
        if 1 <= step <= NCH:
            y_finish(step - 1)
        if step >= 2:
            z_finish(step - 2)
    for c in sends:
        c.wait_send()


def solution(mesh):
    def step(snapshots, steering, combining, beam_list):
        snaps, _, _, elements = snapshots.shape
        partial = steering.shape[3]
        beams = combining.shape[3]
        width = beams // NCH
        dma = pltpu.SemaphoreType.DMA
        out = pl.pallas_call(
            kernel,
            out_shape=jax.ShapeDtypeStruct((16, beams), BF),
            in_specs=[
                pl.BlockSpec(memory_space=pl.ANY),
                pl.BlockSpec(memory_space=pl.ANY),
                pl.BlockSpec(memory_space=pl.ANY),
                pl.BlockSpec(memory_space=pltpu.VMEM),
            ],
            out_specs=pl.BlockSpec(memory_space=pltpu.VMEM),
            scratch_shapes=[
                pltpu.VMEM((2 * snaps, elements), BF),
                pltpu.VMEM((2, partial, elements), BF),
                pltpu.VMEM((16, 2, 256, 128), F32),
                pltpu.VMEM((8, 4, 64, 128), BF),
                pltpu.VMEM((8, 4, 64, 128), BF),
                pltpu.VMEM((8, 512, 128), BF),
                pltpu.VMEM((NCH, 8, 2, 64, width), BF),
                pltpu.VMEM((NCH, width, beams), BF),
                pltpu.VMEM((NCH, 4, 8, 16, width), BF),
                pltpu.VMEM((NCH, 2, 4, 16, width), BF),
                pltpu.VMEM((NCH, 2, 4, 16, width), BF),
                pltpu.VMEM((NCH, 2, 8, 16, width), BF),
                pltpu.VMEM((NCH, 8, 16, width), BF),
                pltpu.VMEM((NCH, 8, 16, width), BF),
                pltpu.VMEM((16, beams), F32),
                dma((2,)),
                dma((NCH,)),
                dma((8,)),
                dma((8,)),
                dma((NCH, 8)),
                dma((NCH, 8)),
                dma((NCH, 6)),
                dma((NCH, 6)),
                dma((NCH, 8)),
                dma((NCH, 8)),
            ],
            compiler_params=pltpu.CompilerParams(collective_id=0, has_side_effects=True),
        )(
            snapshots[:, :, 0, :].reshape(2 * snaps, elements),
            jnp.swapaxes(steering[0], 1, 2),
            combining[0],
            beam_list.reshape(1, beams),
        )
        return out.reshape(2, 8, beams)

    placed = (
        P(None, None, ("grp", "sub"), None),
        P(("grp", "sub"), None, None, None),
        P(("grp", "sub"), None, None, None),
        P(),
    )
    return jax.shard_map(
        step, mesh=mesh, in_specs=placed, out_specs=P(None, ("grp", "sub"), None), check_vma=False
    )
```

```python
import jax
import jax.numpy as jnp
from jax import lax
from jax.experimental import pallas as pl
from jax.experimental.pallas import tpu as pltpu
from jax.sharding import PartitionSpec as P

MESH = pl.DeviceIdType.MESH
BF = jnp.bfloat16
F32 = jnp.float32
UNITS = 8
CHUNKS = ((0, 2), (2, 2), (4, 2), (6, 2))


def kernel(
    snap_ref, steer_ref, comb_ref, list_ref, out_ref,
    snap, steer, prod, p_send, p_all, lhs, w_all, sel, part, yrecv, tsum, zrecv, acc,
    load_sem, wload_sem, p_ss, p_rs, w_ss, w_rs, y_ss, y_rs, z_ss, z_rs, ring_sem,
):
    grp = lax.axis_index("grp")
    sub = lax.axis_index("sub")
    zl, core = grp // 2, grp % 2
    x, zh, y = sub // 16, (sub // 4) % 4, sub % 4
    z = zh * 2 + zl
    other = 1 - core
    me = x * 2 + core

    def dev_x(x2, c2):
        return (zl * 2 + c2, x2 * 16 + zh * 4 + y)

    def dev_y(y2):
        return (grp, x * 16 + zh * 4 + y2)

    def dev_z(z2):
        return ((z2 % 2) * 2 + core, x * 16 + (z2 // 2) * 4 + y)

    def zrow(z2):
        return (z2 % 2) * 4 + z2 // 2

    wloads = []
    for u in range(UNITS):
        c = pltpu.make_async_copy(
            comb_ref.at[:, :, pl.ds(u * 128, 128)], w_all.at[u, me], wload_sem.at[u]
        )
        wloads.append(c)
    loads = [
        pltpu.make_async_copy(steer_ref, steer, load_sem.at[0]),
        pltpu.make_async_copy(snap_ref, snap, load_sem.at[1]),
    ]
    for c in wloads[:2] + loads + wloads[2:]:
        c.start()

    barrier = pltpu.get_barrier_semaphore()
    peers = [dev_x((x + dx) % 4, core if dc == 0 else other)
             for dx in range(4) for dc in range(2) if dx or dc]
    peers += [dev_y((y + dy) % 4) for dy in range(1, 4)]
    peers += [dev_z((z + dz) % 8) for dz in (1, 7)]
    for p in peers:
        pl.semaphore_signal(barrier, inc=1, device_id=p, device_id_type=MESH)

    sends = []

    def remote(src, dst, ss, rs, dev):
        return pltpu.make_async_remote_copy(
            src_ref=src, dst_ref=dst, send_sem=ss, recv_sem=rs, device_id=dev, device_id_type=MESH
        )

    def send(src, dst, ss, rs, dev):
        c = remote(src, dst, ss, rs, dev)
        c.start()
        sends.append(c)

    def arrived(dst, ss, rs, dev):
        remote(dst, dst, ss, rs, dev).wait_recv()

    def ring_signal(k, hop):
        for j, d in enumerate((hop, 8 - hop)):
            pl.semaphore_signal(
                ring_sem.at[k, j], inc=1, device_id=dev_z((z + d) % 8), device_id_type=MESH
            )

    def ring_wait(k):
        for j in range(2):
            pl.semaphore_wait(ring_sem.at[k, j], 1)

    def w_own(ch):
        u, n = CHUNKS[ch]
        for k in range(u, u + n):
            wloads[k].wait()
        mine = w_all.at[pl.ds(u, n), me]
        for dx in (2, 1, 3):
            send(mine, mine, w_ss.at[ch, dx], w_rs.at[ch, dx], dev_x((x + dx) % 4, core))
        send(mine, mine, w_ss.at[ch, 4], w_rs.at[ch, 4], dev_x(x, other))

    def w_forward(ch):
        u, n = CHUNKS[ch]
        for dx in (1, 3, 2):
            x2 = (x + 4 - dx) % 4
            a = w_all.at[pl.ds(u, n), x2 * 2 + core]
            arrived(a, w_ss.at[ch, dx], w_rs.at[ch, dx], dev_x(x2, core))
            send(a, a, w_ss.at[ch, 4 + dx], w_rs.at[ch, 4 + dx], dev_x(x, other))

    def w_finish(ch):
        u, n = CHUNKS[ch]
        for dx in (0, 1, 3, 2):
            x2 = (x + 4 - dx) % 4
            a = w_all.at[pl.ds(u, n), x2 * 2 + other]
            arrived(a, w_ss.at[ch, 4 + dx], w_rs.at[ch, 4 + dx], dev_x(x, other))

    order = [(2, 0), (2, 1), (1, 0), (3, 0), (1, 1), (3, 1), (0, 1), (0, 0)]

    def first_section():
        for c in loads:
            c.wait()
        s_re, s_im = steer[0], steer[1]
        weights = jnp.concatenate([s_re, s_im, -s_im, s_re], axis=0)
        for n, (dx, dc) in enumerate(order):
            x2 = (x + dx) % 4
            c2 = core if dc == 0 else other
            dest = x2 * 2 + c2
            for half in range(2):
                block = half * 8 + c2 * 4 + x2
                rows = snap[pl.ds(pl.multiple_of(block * 256, 256), 256), :]
                slot = n * 2 + half
                both = lax.dot_general(
                    rows, weights, (((1,), (1,)), ((), ())), preferred_element_type=F32
                )
                prod[slot, 0] = both[:, :128]
                prod[slot, 1] = both[:, 128:]
                val = prod[slot, 0, pl.ds(0, 128, stride=2)] + prod[slot, 1, pl.ds(1, 128, stride=2)]
                for q in range(4):
                    got = jnp.concatenate(
                        [val[h * 32 + q * 8 : h * 32 + q * 8 + 8] for h in range(4)], axis=0
                    )
                    p_send[dest, q, pl.ds(half * 32, 32), :] = got.astype(BF)

    def p_sends():
        for dx, dc in order[:-1]:
            x2 = (x + dx) % 4
            c2 = core if dc == 0 else other
            r = dx * 2 + dc
            send(p_send.at[x2 * 2 + c2], p_all.at[me], p_ss.at[r], p_rs.at[r], dev_x(x2, c2))

    def build_lhs():
        sign = jnp.where(lax.broadcasted_iota(jnp.int32, (256, 128), 1) < 64, 1.0, -1.0)
        for dx, dc in [(0, 0)] + order[:-1]:
            x2 = (x + 4 - dx) % 4
            c2 = core if dc == 0 else other
            src = x2 * 2 + c2
            if dx or dc:
                r = dx * 2 + dc
                arrived(p_all.at[src], p_ss.at[r], p_rs.at[r], dev_x(x2, c2))
                val = p_all[src]
            else:
                val = p_send[src]
            val = val.reshape(256, 128).astype(F32)
            top = (val * sign).reshape(32, 8, 128)
            low = pltpu.roll(val, 64, 1).reshape(32, 8, 128)
            lhs[src] = jnp.concatenate([top, low], axis=1).astype(BF).reshape(512, 128)

    def multiply(ch):
        u, n = CHUNKS[ch]
        left = jnp.concatenate([lhs[k] for k in range(8)], axis=1)
        right = jnp.concatenate([w_all[k].reshape(1024, 128) for k in range(u, u + n)], axis=1)
        val = jnp.dot(left, right, preferred_element_type=F32)
        for k in range(n):
            part[u + k] = val[:, k * 128 : k * 128 + 128].astype(BF).reshape(4, 8, 16, 128)

    def y_send(ch):
        u, n = CHUNKS[ch]
        for dy in (2, 1, 3):
            y2 = (y + dy) % 4
            send(part.at[pl.ds(u, n), y2], yrecv.at[pl.ds(u, n), dy], y_ss.at[ch, dy], y_rs.at[ch, dy], dev_y(y2))

    def y_finish(ch):
        u, n = CHUNKS[ch]
        for dy in (1, 3, 2):
            arrived(yrecv.at[pl.ds(u, n), dy], y_ss.at[ch, dy], y_rs.at[ch, dy], dev_y((y + dy) % 4))
        for k in range(u, u + n):
            total = part[k, y].astype(F32)
            for dy in (1, 3, 2):
                total = total + yrecv[k, dy].astype(F32)
            tsum[k] = total.astype(BF)

    def z_send(ch):
        u, n = CHUNKS[ch]
        for dz in (4, 3, 5, 2, 6, 1, 7):
            z2 = (z + dz) % 8
            send(tsum.at[pl.ds(u, n), zrow(z2)], zrecv.at[pl.ds(u, n), dz], z_ss.at[ch, dz], z_rs.at[ch, dz], dev_z(z2))

    def z_finish(ch):
        u, n = CHUNKS[ch]
        for dz in range(1, 8):
            arrived(zrecv.at[pl.ds(u, n), dz], z_ss.at[ch, dz], z_rs.at[ch, dz], dev_z((z + dz) % 8))
        mine = zrow(z)
        got = []
        for k in range(u, u + n):
            total = tsum[k, mine].astype(F32)
            for dz in range(1, 8):
                total = total + zrecv[k, dz].astype(F32)
            got.append(total.astype(BF))
        val = jnp.dot(
            jnp.concatenate(got, axis=1), sel[pl.ds(u * 128, n * 128)], preferred_element_type=F32
        )
        if ch == 0:
            acc[...] = val
        elif ch < len(CHUNKS) - 1:
            acc[...] += val
        else:
            out_ref[...] = (acc[...] + val).astype(BF)

    last = len(CHUNKS)
    with jax.named_scope("barrier"):
        pl.semaphore_wait(barrier, len(peers))
    with jax.named_scope("start"):
        ring_signal(0, 1)
        w_own(0)
    with jax.named_scope("first"):
        first_section()
    with jax.named_scope("psend"):
        p_sends()
    with jax.named_scope("w_own"):
        for ch in range(1, last):
            w_own(ch)
    with jax.named_scope("sel"):
        for ch in range(UNITS // 2):
            rows = lax.broadcasted_iota(jnp.int32, (256, 1024), 0) + ch * 256
            sel[pl.ds(ch * 256, 256)] = jnp.where(rows == list_ref[...], 1.0, 0.0).astype(BF)
    with jax.named_scope("ring"):
        ring_wait(0)
        ring_signal(1, 2)
    with jax.named_scope("w_forward_0"):
        w_forward(0)
    with jax.named_scope("lhs"):
        build_lhs()
    with jax.named_scope("ringwait"):
        ring_wait(1)
    for step in range(last + 3):
        if step < last:
            if step:
                with jax.named_scope(f"w_forward_{step}"):
                    w_forward(step)
        if 2 <= step <= last + 1:
            with jax.named_scope(f"y_finish_{step-2}"):
                y_finish(step - 2)
            with jax.named_scope(f"z_send_{step-2}"):
                z_send(step - 2)
        if step < last:
            with jax.named_scope(f"w_finish_{step}"):
                w_finish(step)
            with jax.named_scope(f"mult_{step}"):
                multiply(step)
            with jax.named_scope(f"y_send_{step}"):
                y_send(step)
        if step >= 3:
            with jax.named_scope(f"z_finish_{step-3}"):
                z_finish(step - 3)
    with jax.named_scope("sends"):
        for c in sends:
            c.wait_send()


def solution(mesh):
    def step(snapshots, steering, combining, beam_list):
        snaps, _, _, elements = snapshots.shape
        partial = steering.shape[3]
        beams = combining.shape[3]
        dma = pltpu.SemaphoreType.DMA
        chunks = len(CHUNKS)
        out = pl.pallas_call(
            kernel,
            out_shape=jax.ShapeDtypeStruct((16, beams), BF),
            in_specs=[
                pl.BlockSpec(memory_space=pl.ANY),
                pl.BlockSpec(memory_space=pl.ANY),
                pl.BlockSpec(memory_space=pl.ANY),
                pl.BlockSpec(memory_space=pltpu.VMEM),
            ],
            out_specs=pl.BlockSpec(memory_space=pltpu.VMEM),
            scratch_shapes=[
                pltpu.VMEM((2 * snaps, elements), BF),
                pltpu.VMEM((2, partial, elements), BF),
                pltpu.VMEM((16, 2, 256, 128), F32),
                pltpu.VMEM((8, 4, 64, 128), BF),
                pltpu.VMEM((8, 4, 64, 128), BF),
                pltpu.VMEM((8, 512, 128), BF),
                pltpu.VMEM((UNITS, 8, 2, 64, 128), BF),
                pltpu.VMEM((beams, beams), BF),
                pltpu.VMEM((UNITS, 4, 8, 16, 128), BF),
                pltpu.VMEM((UNITS, 4, 8, 16, 128), BF),
                pltpu.VMEM((UNITS, 8, 16, 128), BF),
                pltpu.VMEM((UNITS, 8, 16, 128), BF),
                pltpu.VMEM((16, beams), F32),
                dma((2,)),
                dma((UNITS,)),
                dma((8,)),
                dma((8,)),
                dma((chunks, 8)),
                dma((chunks, 8)),
                dma((chunks, 4)),
                dma((chunks, 4)),
                dma((chunks, 8)),
                dma((chunks, 8)),
                pltpu.SemaphoreType.REGULAR((2, 2)),
            ],
            compiler_params=pltpu.CompilerParams(collective_id=0, has_side_effects=True),
        )(
            snapshots[:, :, 0, :].reshape(2 * snaps, elements),
            jnp.swapaxes(steering[0], 1, 2),
            combining[0],
            beam_list.reshape(1, beams),
        )
        return out.reshape(2, 8, beams)

    placed = (
        P(None, None, ("grp", "sub"), None),
        P(("grp", "sub"), None, None, None),
        P(("grp", "sub"), None, None, None),
        P(),
    )
    return jax.shard_map(
        step, mesh=mesh, in_specs=placed, out_specs=P(None, ("grp", "sub"), None), check_vma=False
    )
```

```python
import jax
import jax.numpy as jnp
from jax import lax
from jax.experimental import pallas as pl
from jax.experimental.pallas import tpu as pltpu
from jax.sharding import PartitionSpec as P

MESH = pl.DeviceIdType.MESH
BF = jnp.bfloat16
F32 = jnp.float32
UNITS = 8
CHUNKS = ((0, 0, 1), (1, 4, 1), (0, 1, 1), (1, 5, 1), (0, 2, 1), (1, 6, 1), (0, 3, 1), (1, 7, 1))
LAG_R = 5


def kernel(
    snap_ref, steer_ref, comb_ref, list_ref, out_ref,
    snap, steer, order_row, prod, p_send, p_all, lhs, w_all, sel, part, rrecv, tsum, zrecv, acc,
    load_sem, wload_sem, p_rs, w_rs, r_rs, z_rs, sent, ring_sem,
):
    grp = lax.axis_index("grp")
    sub = lax.axis_index("sub")
    zl, core = grp // 2, grp % 2
    x, zh, y = sub // 16, (sub // 4) % 4, sub % 4
    z = zh * 2 + zl
    other = 1 - core
    gat, red = (x, y), (y, x)
    me = (x * 2 + core, y * 2 + core)

    def dev_g(o, d, c2):
        if o == 0:
            return (zl * 2 + c2, ((x + d) % 4) * 16 + zh * 4 + y)
        return (zl * 2 + c2, x * 16 + zh * 4 + (y + d) % 4)

    def dev_r(o, d):
        return dev_g(1 - o, d, core)

    def dev_z(z2):
        return ((z2 % 2) * 2 + core, x * 16 + (z2 // 2) * 4 + y)

    def zrow(z2):
        return (z2 % 2) * 4 + z2 // 2

    owner = {}
    for o, u, n in CHUNKS:
        for k in range(u, u + n):
            owner[k] = o
    wloads = []
    for u in range(UNITS):
        c = pltpu.make_async_copy(
            comb_ref.at[:, :, pl.ds(u * 128, 128)], w_all.at[u, me[owner[u]]], wload_sem.at[u]
        )
        wloads.append(c)
    loads = [
        pltpu.make_async_copy(steer_ref, steer, load_sem.at[0]),
        pltpu.make_async_copy(snap_ref, snap, load_sem.at[1]),
        pltpu.make_async_copy(list_ref, order_row, load_sem.at[2]),
    ]
    early = [k for _, u, n in CHUNKS[:2] for k in range(u, u + n)]
    late = [k for k in range(UNITS) if k not in early]
    for c in [wloads[k] for k in early] + loads + [wloads[k] for k in late]:
        c.start()

    barrier = pltpu.get_barrier_semaphore()
    peers = [dev_g(o, d, c2) for o in range(2) for d in range(1, 4) for c2 in (core, other)]
    peers += [dev_g(0, 0, other)]
    peers += [dev_z((z + dz) % 8) for dz in (1, 7)]
    for p in peers:
        pl.semaphore_signal(barrier, inc=1, device_id=p, device_id_type=MESH)

    def send(kind, src, dst, rs, dev):
        pltpu.make_async_remote_copy(
            src_ref=src, dst_ref=dst, send_sem=sent.at[kind], recv_sem=rs, device_id=dev,
            device_id_type=MESH,
        ).start()

    def arrived(ref, rs):
        pltpu.make_async_copy(ref, ref, rs).wait()

    def ring_signal(k, hop):
        for j, d in enumerate((hop, 8 - hop)):
            pl.semaphore_signal(
                ring_sem.at[k, j], inc=1, device_id=dev_z((z + d) % 8), device_id_type=MESH
            )

    def ring_wait(k):
        for j in range(2):
            pl.semaphore_wait(ring_sem.at[k, j], 1)

    def w_own(ch):
        o, u, n = CHUNKS[ch]
        for k in range(u, u + n):
            wloads[k].wait()
        mine = w_all.at[pl.ds(u, n), me[o]]
        for d in (2, 1, 3):
            send(0, mine, mine, w_rs.at[ch, 0], dev_g(o, d, core))
        send(0, mine, mine, w_rs.at[ch, 1], dev_g(o, 0, other))

    def w_forward(ch):
        o, u, n = CHUNKS[ch]
        got = [w_all.at[pl.ds(u, n), ((gat[o] + 4 - d) % 4) * 2 + core] for d in (1, 3, 2)]
        arrived(w_all.at[pl.ds(u, n), pl.ds(0, 3)], w_rs.at[ch, 0])
        for a in got:
            send(0, a, a, w_rs.at[ch, 1], dev_g(o, 0, other))

    def w_finish(ch):
        o, u, n = CHUNKS[ch]
        arrived(w_all.at[pl.ds(u, n), pl.ds(0, 4)], w_rs.at[ch, 1])

    order = [(2, 0), (2, 1), (1, 0), (3, 0), (1, 1), (3, 1), (0, 1)]

    def first_section():
        for c in loads:
            c.wait()
        s_re, s_im = steer[0], steer[1]
        weights = jnp.concatenate([s_re, s_im, -s_im, s_re], axis=0)
        for half in range(2):
            for c2 in range(2):
                for x2 in range(4):
                    slot = half * 8 + c2 * 4 + x2
                    rows = snap[slot * 256 : slot * 256 + 256, :]
                    both = lax.dot_general(
                        rows, weights, (((1,), (1,)), ((), ())), preferred_element_type=F32
                    )
                    prod[slot, 0] = both[:, :128]
                    prod[slot, 1] = both[:, 128:]
                    val = (
                        prod[slot, 0, pl.ds(0, 128, stride=2)]
                        + prod[slot, 1, pl.ds(1, 128, stride=2)]
                    )
                    for q in range(4):
                        got = jnp.concatenate(
                            [val[h * 32 + q * 8 : h * 32 + q * 8 + 8] for h in range(4)], axis=0
                        ).astype(BF)
                        p_send[0, x2 * 2 + c2, q, half * 32 : half * 32 + 32, :] = got
                        p_send[1, q * 2 + c2, x2, half * 32 : half * 32 + 32, :] = got

    def p_sends():
        for d, dc in order:
            for o in range(2):
                c2 = core if dc == 0 else other
                dest = ((gat[o] + d) % 4) * 2 + c2
                send(1, p_send.at[o, dest], p_all.at[o, me[o]], p_rs.at[o, d], dev_g(o, d, c2))

    def build_lhs(o):
        sign = jnp.where(lax.broadcasted_iota(jnp.int32, (256, 128), 1) < 64, 1.0, -1.0)
        for d, dc in [(0, 0), (0, 1), (1, 0), (1, 1), (3, 0), (3, 1), (2, 0), (2, 1)]:
            c2 = core if dc == 0 else other
            base = ((gat[o] + 4 - d) % 4) * 2
            src = base + c2
            if d == 0 and dc:
                arrived(p_all.at[o, src], p_rs.at[o, d])
            elif d and dc == 0:
                arrived(p_all.at[o, pl.ds(base, 2)], p_rs.at[o, d])
            val = p_all[o, src] if d or dc else p_send[o, src]
            val = val.reshape(256, 128).astype(F32)
            top = (val * sign).reshape(32, 8, 128)
            low = pltpu.roll(val, 64, 1).reshape(32, 8, 128)
            lhs[o, src] = jnp.concatenate([top, low], axis=1).astype(BF).reshape(512, 128)

    def multiply(ch):
        o, u, n = CHUNKS[ch]
        left = jnp.concatenate([lhs[o, k] for k in range(8)], axis=1)
        right = jnp.concatenate([w_all[k].reshape(1024, 128) for k in range(u, u + n)], axis=1)
        val = jnp.dot(left, right, preferred_element_type=F32)
        for k in range(n):
            part[u + k] = val[:, k * 128 : k * 128 + 128].astype(BF).reshape(4, 8, 16, 128)

    def r_send(ch):
        o, u, n = CHUNKS[ch]
        for d in (2, 1, 3):
            send(
                2, part.at[pl.ds(u, n), (red[o] + d) % 4], rrecv.at[pl.ds(u, n), d],
                r_rs.at[ch], dev_r(o, d),
            )

    def r_finish(ch):
        o, u, n = CHUNKS[ch]
        arrived(rrecv.at[pl.ds(u, n), pl.ds(1, 3)], r_rs.at[ch])
        for k in range(u, u + n):
            total = part[k, red[o]].astype(F32)
            for d in (1, 3, 2):
                total = total + rrecv[k, d].astype(F32)
            tsum[k] = total.astype(BF)

    def z_send(ch):
        o, u, n = CHUNKS[ch]
        for dz in (4, 3, 5, 2, 6, 1, 7):
            z2 = (z + dz) % 8
            send(
                3, tsum.at[pl.ds(u, n), zrow(z2)], zrecv.at[pl.ds(u, n), dz],
                z_rs.at[ch], dev_z(z2),
            )

    def z_finish(ch):
        o, u, n = CHUNKS[ch]
        arrived(zrecv.at[pl.ds(u, n), pl.ds(1, 7)], z_rs.at[ch])
        mine = zrow(z)
        got = []
        for k in range(u, u + n):
            total = tsum[k, mine].astype(F32)
            for dz in range(1, 8):
                total = total + zrecv[k, dz].astype(F32)
            got.append(total.astype(BF))
        val = jnp.dot(
            jnp.concatenate(got, axis=1), sel[pl.ds(u * 128, n * 128)], preferred_element_type=F32
        )
        if ch == 0:
            acc[...] = val
        elif ch < len(CHUNKS) - 1:
            acc[...] += val
        else:
            out_ref[...] = (acc[...] + val).astype(BF)

    last = len(CHUNKS)
    scope = jax.named_scope
    with scope("barrier"):
        pl.semaphore_wait(barrier, len(peers))
    with scope("start"):
        ring_signal(0, 1)
        w_own(0)
        w_own(1)
    with scope("first"):
        first_section()
    with scope("psend"):
        p_sends()
    with scope("w_own"):
        for ch in range(2, last):
            w_own(ch)
    with scope("sel"):
        for k in range(UNITS // 2):
            rows = lax.broadcasted_iota(jnp.int32, (256, 1024), 0) + k * 256
            sel[pl.ds(k * 256, 256)] = jnp.where(rows == order_row[...], 1.0, 0.0).astype(BF)
    with scope("ring"):
        ring_wait(0)
        ring_signal(1, 2)
    with scope("w_forward_0"):
        w_forward(0)
        w_forward(1)
    with scope("lhs"):
        build_lhs(0)
        build_lhs(1)
    with scope("ringwait"):
        ring_wait(1)
    for step in range(last + LAG_R):
        if 0 < step and step + 1 < last:
            with scope(f"w_forward_{step+1}"):
                w_forward(step + 1)
        if step < last:
            with scope(f"w_finish_{step}"):
                w_finish(step)
            with scope(f"mult_{step}"):
                multiply(step)
            with scope(f"r_send_{step}"):
                r_send(step)
        if 0 <= step - LAG_R < last:
            with scope(f"r_finish_{step-LAG_R}"):
                r_finish(step - LAG_R)
            with scope(f"z_send_{step-LAG_R}"):
                z_send(step - LAG_R)
    for ch in range(last):
        with scope(f"z_finish_{ch}"):
            z_finish(ch)
    with scope("sends"):
        arrived(w_all.at[:, pl.ds(0, 7)], sent.at[0])
        arrived(p_all.at[:, pl.ds(0, 7)], sent.at[1])
        arrived(rrecv.at[:, pl.ds(0, 3)], sent.at[2])
        arrived(zrecv.at[:, pl.ds(0, 7)], sent.at[3])


def solution(mesh):
    def step(snapshots, steering, combining, beam_list):
        snaps, _, _, elements = snapshots.shape
        partial = steering.shape[3]
        beams = combining.shape[3]
        dma = pltpu.SemaphoreType.DMA
        chunks = len(CHUNKS)
        out = pl.pallas_call(
            kernel,
            out_shape=jax.ShapeDtypeStruct((16, beams), BF),
            in_specs=[
                pl.BlockSpec(memory_space=pl.ANY),
                pl.BlockSpec(memory_space=pl.ANY),
                pl.BlockSpec(memory_space=pl.ANY),
                pl.BlockSpec(memory_space=pl.ANY),
            ],
            out_specs=pl.BlockSpec(memory_space=pltpu.VMEM),
            scratch_shapes=[
                pltpu.VMEM((2 * snaps, elements), BF),
                pltpu.VMEM((2, partial, elements), BF),
                pltpu.VMEM((1, beams), jnp.int32),
                pltpu.VMEM((16, 2, 256, 128), F32),
                pltpu.VMEM((2, 8, 4, 64, 128), BF),
                pltpu.VMEM((2, 8, 4, 64, 128), BF),
                pltpu.VMEM((2, 8, 512, 128), BF),
                pltpu.VMEM((UNITS, 8, 2, 64, 128), BF),
                pltpu.VMEM((beams, beams), BF),
                pltpu.VMEM((UNITS, 4, 8, 16, 128), BF),
                pltpu.VMEM((UNITS, 4, 8, 16, 128), BF),
                pltpu.VMEM((UNITS, 8, 16, 128), BF),
                pltpu.VMEM((UNITS, 8, 16, 128), BF),
                pltpu.VMEM((16, beams), F32),
                dma((3,)),
                dma((UNITS,)),
                dma((2, 4)),
                dma((chunks, 2)),
                dma((chunks,)),
                dma((chunks,)),
                dma((4,)),
                pltpu.SemaphoreType.REGULAR((2, 2)),
            ],
            compiler_params=pltpu.CompilerParams(collective_id=0, has_side_effects=True),
        )(
            snapshots[:, :, 0, :].reshape(2 * snaps, elements),
            jnp.swapaxes(steering[0], 1, 2),
            combining[0],
            beam_list.reshape(1, beams),
        )
        return out.reshape(2, 8, beams)

    placed = (
        P(None, None, ("grp", "sub"), None),
        P(("grp", "sub"), None, None, None),
        P(("grp", "sub"), None, None, None),
        P(),
    )
    return jax.shard_map(
        step, mesh=mesh, in_specs=placed, out_specs=P(None, ("grp", "sub"), None), check_vma=False
    )
```

```python
import jax
import jax.numpy as jnp
from jax import lax
from jax.experimental import pallas as pl
from jax.experimental.pallas import tpu as pltpu
from jax.sharding import PartitionSpec as P

MESH = pl.DeviceIdType.MESH
BF = jnp.bfloat16
F32 = jnp.float32
UNITS = 8
ORDER = "m0 f1 f5 m4 f2 f6 m1 m5 f3 f7 m2 m6 r0 r4 m3 m7 r1 r5 r2 r6 r3 r7"


def kernel(
    snap_ref, steer_ref, comb_ref, list_ref, out_ref,
    snap, steer, order_row, prod, p_send, p_all, lhs, w_all, sel, part, rrecv, tsum, zrecv, acc,
    load_sem, wload_sem, p_rs, w_rs, r_rs, z_rs, sent, ring_sem,
):
    grp = lax.axis_index("grp")
    sub = lax.axis_index("sub")
    zl, core = grp // 2, grp % 2
    x, zh, y = sub // 16, (sub // 4) % 4, sub % 4
    z = zh * 2 + zl
    other = 1 - core
    gat, red = (x, y), (y, x)
    me = (x * 2 + core, y * 2 + core)

    def dev_g(o, d, c2):
        if o == 0:
            return (zl * 2 + c2, ((x + d) % 4) * 16 + zh * 4 + y)
        return (zl * 2 + c2, x * 16 + zh * 4 + (y + d) % 4)

    def dev_r(o, d):
        return dev_g(1 - o, d, core)

    def dev_z(z2):
        return ((z2 % 2) * 2 + core, x * 16 + (z2 // 2) * 4 + y)

    def zrow(z2):
        return (z2 % 2) * 4 + z2 // 2

    wloads = []
    for u in range(UNITS):
        c = pltpu.make_async_copy(
            comb_ref.at[:, :, pl.ds(u * 128, 128)], w_all.at[u, me[u // 4]], wload_sem.at[u]
        )
        wloads.append(c)
    loads = [
        pltpu.make_async_copy(steer_ref, steer, load_sem.at[0]),
        pltpu.make_async_copy(snap_ref, snap, load_sem.at[1]),
        pltpu.make_async_copy(list_ref, order_row, load_sem.at[2]),
    ]
    for c in [wloads[0], wloads[4]] + loads + [wloads[k] for k in (1, 5, 2, 6, 3, 7)]:
        c.start()

    barrier = pltpu.get_barrier_semaphore()
    peers = [dev_g(o, d, c2) for o in range(2) for d in range(1, 4) for c2 in (core, other)]
    peers += [dev_g(0, 0, other)]
    peers += [dev_z((z + dz) % 8) for dz in (1, 7)]
    for p in peers:
        pl.semaphore_signal(barrier, inc=1, device_id=p, device_id_type=MESH)

    def send(kind, src, dst, rs, dev):
        pltpu.make_async_remote_copy(
            src_ref=src, dst_ref=dst, send_sem=sent.at[kind], recv_sem=rs, device_id=dev,
            device_id_type=MESH,
        ).start()

    def arrived(ref, rs):
        pltpu.make_async_copy(ref, ref, rs).wait()

    def ring_signal(k, hop):
        for j, d in enumerate((hop, 8 - hop)):
            pl.semaphore_signal(
                ring_sem.at[k, j], inc=1, device_id=dev_z((z + d) % 8), device_id_type=MESH
            )

    def ring_wait(k):
        for j in range(2):
            pl.semaphore_wait(ring_sem.at[k, j], 1)

    def w_own(u):
        o = u // 4
        wloads[u].wait()
        mine = w_all.at[u, me[o]]
        for d in (2, 1, 3):
            send(0, mine, mine, w_rs.at[u, 0], dev_g(o, d, core))
        send(0, mine, mine, w_rs.at[u, 1], dev_g(o, 0, other))

    def w_forward(u):
        o = u // 4
        arrived(w_all.at[u, pl.ds(0, 3)], w_rs.at[u, 0])
        for d in (1, 3, 2):
            a = w_all.at[u, ((gat[o] + 4 - d) % 4) * 2 + core]
            send(0, a, a, w_rs.at[u, 1], dev_g(o, 0, other))

    order = [(2, 0), (2, 1), (1, 0), (3, 0), (1, 1), (3, 1), (0, 1)]

    def first_section():
        for c in loads:
            c.wait()
        s_re, s_im = steer[0], steer[1]
        weights = jnp.concatenate([s_re, s_im, -s_im, s_re], axis=0)
        for half in range(2):
            for c2 in range(2):
                for x2 in range(4):
                    slot = half * 8 + c2 * 4 + x2
                    rows = snap[slot * 256 : slot * 256 + 256, :]
                    both = lax.dot_general(
                        rows, weights, (((1,), (1,)), ((), ())), preferred_element_type=F32
                    )
                    prod[slot, 0] = both[:, :128]
                    prod[slot, 1] = both[:, 128:]
                    val = (
                        prod[slot, 0, pl.ds(0, 128, stride=2)]
                        + prod[slot, 1, pl.ds(1, 128, stride=2)]
                    )
                    for q in range(4):
                        got = jnp.concatenate(
                            [val[h * 32 + q * 8 : h * 32 + q * 8 + 8] for h in range(4)], axis=0
                        ).astype(BF)
                        p_send[0, x2 * 2 + c2, q, half * 32 : half * 32 + 32, :] = got
                        p_send[1, q * 2 + c2, x2, half * 32 : half * 32 + 32, :] = got

    def p_sends():
        for d, dc in order:
            for o in range(2):
                c2 = core if dc == 0 else other
                dest = ((gat[o] + d) % 4) * 2 + c2
                send(1, p_send.at[o, dest], p_all.at[o, me[o]], p_rs.at[o, d], dev_g(o, d, c2))

    def build_lhs(o):
        sign = jnp.where(lax.broadcasted_iota(jnp.int32, (256, 128), 1) < 64, 1.0, -1.0)
        for d, dc in [(0, 0), (0, 1), (1, 0), (1, 1), (3, 0), (3, 1), (2, 0), (2, 1)]:
            c2 = core if dc == 0 else other
            base = ((gat[o] + 4 - d) % 4) * 2
            src = base + c2
            if d == 0 and dc:
                arrived(p_all.at[o, src], p_rs.at[o, d])
            elif d and dc == 0:
                arrived(p_all.at[o, pl.ds(base, 2)], p_rs.at[o, d])
            val = p_all[o, src] if d or dc else p_send[o, src]
            val = val.reshape(256, 128).astype(F32)
            top = (val * sign).reshape(32, 8, 128)
            low = pltpu.roll(val, 64, 1).reshape(32, 8, 128)
            lhs[o, src] = jnp.concatenate([top, low], axis=1).astype(BF).reshape(512, 128)

    def multiply(units):
        o = units[0] // 4
        for u in units:
            arrived(w_all.at[u, pl.ds(0, 4)], w_rs.at[u, 1])
        left = jnp.concatenate([lhs[o, k] for k in range(8)], axis=1)
        right = jnp.concatenate([w_all[u].reshape(1024, 128) for u in units], axis=1)
        val = jnp.dot(left, right, preferred_element_type=F32)
        for n, u in enumerate(units):
            part[u] = val[:, n * 128 : n * 128 + 128].astype(BF).reshape(4, 8, 16, 128)
        for u in units:
            for d in (2, 1, 3):
                send(2, part.at[u, (red[o] + d) % 4], rrecv.at[u, d], r_rs.at[u], dev_r(o, d))

    def r_finish(u):
        arrived(rrecv.at[u, pl.ds(1, 3)], r_rs.at[u])
        total = part[u, red[u // 4]].astype(F32)
        for d in (1, 3, 2):
            total = total + rrecv[u, d].astype(F32)
        tsum[u] = total.astype(BF)
        for dz in (4, 3, 5, 2, 6, 1, 7):
            z2 = (z + dz) % 8
            send(3, tsum.at[u, zrow(z2)], zrecv.at[u, dz], z_rs.at[u], dev_z(z2))

    def z_finish(u):
        arrived(zrecv.at[u, pl.ds(1, 7)], z_rs.at[u])
        total = tsum[u, zrow(z)].astype(F32)
        for dz in range(1, 8):
            total = total + zrecv[u, dz].astype(F32)
        return jnp.dot(
            total.astype(BF), sel[pl.ds(u * 128, 128)], preferred_element_type=F32
        )

    scope = jax.named_scope
    with scope("barrier"):
        pl.semaphore_wait(barrier, len(peers))
    with scope("start"):
        ring_signal(0, 1)
        w_own(0)
        w_own(4)
    with scope("first"):
        first_section()
    with scope("psend"):
        p_sends()
    with scope("w_own"):
        for u in (1, 5, 2, 6, 3, 7):
            w_own(u)
    with scope("sel"):
        for k in range(UNITS // 2):
            rows = lax.broadcasted_iota(jnp.int32, (256, 1024), 0) + k * 256
            sel[pl.ds(k * 256, 256)] = jnp.where(rows == order_row[...], 1.0, 0.0).astype(BF)
    with scope("ring"):
        ring_wait(0)
        ring_signal(1, 2)
    with scope("w_forward_0"):
        w_forward(0)
        w_forward(4)
    with scope("lhs"):
        build_lhs(0)
        build_lhs(1)
    with scope("ringwait"):
        ring_wait(1)
    sums = []
    for op in ORDER.split():
        units = [int(k) for k in op[1:]]
        with scope(op):
            if op[0] == "f":
                w_forward(units[0])
            elif op[0] == "m":
                multiply(units)
            else:
                r_finish(units[0])
                sums.append(units[0])
    for n, u in enumerate(sums):
        with scope(f"z{u}"):
            val = z_finish(u)
            if n == 0:
                acc[...] = val
            elif n < UNITS - 1:
                acc[...] += val
            else:
                out_ref[...] = (acc[...] + val).astype(BF)
    with scope("sends"):
        arrived(w_all.at[:, pl.ds(0, 7)], sent.at[0])
        arrived(p_all.at[:, pl.ds(0, 7)], sent.at[1])
        arrived(rrecv.at[:, pl.ds(0, 3)], sent.at[2])
        arrived(zrecv.at[:, pl.ds(0, 7)], sent.at[3])


def solution(mesh):
    def step(snapshots, steering, combining, beam_list):
        snaps, _, _, elements = snapshots.shape
        partial = steering.shape[3]
        beams = combining.shape[3]
        dma = pltpu.SemaphoreType.DMA
        out = pl.pallas_call(
            kernel,
            out_shape=pltpu.VMEM((16, beams), BF),
            in_specs=[
                pl.BlockSpec(memory_space=pl.ANY),
                pl.BlockSpec(memory_space=pl.ANY),
                pl.BlockSpec(memory_space=pl.ANY),
                pl.BlockSpec(memory_space=pl.ANY),
            ],
            out_specs=pl.BlockSpec(memory_space=pltpu.VMEM),
            scratch_shapes=[
                pltpu.VMEM((2 * snaps, elements), BF),
                pltpu.VMEM((2, partial, elements), BF),
                pltpu.VMEM((1, beams), jnp.int32),
                pltpu.VMEM((16, 2, 256, 128), F32),
                pltpu.VMEM((2, 8, 4, 64, 128), BF),
                pltpu.VMEM((2, 8, 4, 64, 128), BF),
                pltpu.VMEM((2, 8, 512, 128), BF),
                pltpu.VMEM((UNITS, 8, 2, 64, 128), BF),
                pltpu.VMEM((beams, beams), BF),
                pltpu.VMEM((UNITS, 4, 8, 16, 128), BF),
                pltpu.VMEM((UNITS, 4, 8, 16, 128), BF),
                pltpu.VMEM((UNITS, 8, 16, 128), BF),
                pltpu.VMEM((UNITS, 8, 16, 128), BF),
                pltpu.VMEM((16, beams), F32),
                dma((3,)),
                dma((UNITS,)),
                dma((2, 4)),
                dma((UNITS, 2)),
                dma((UNITS,)),
                dma((UNITS,)),
                dma((4,)),
                pltpu.SemaphoreType.REGULAR((2, 2)),
            ],
            compiler_params=pltpu.CompilerParams(collective_id=0, has_side_effects=True),
        )(
            snapshots[:, :, 0, :].reshape(2 * snaps, elements),
            jnp.swapaxes(steering[0], 1, 2),
            combining[0],
            beam_list.reshape(1, beams),
        )
        return out.reshape(2, 8, beams)

    placed = (
        P(None, None, ("grp", "sub"), None),
        P(("grp", "sub"), None, None, None),
        P(("grp", "sub"), None, None, None),
        P(),
    )
    return jax.shard_map(
        step, mesh=mesh, in_specs=placed, out_specs=P(None, ("grp", "sub"), None), check_vma=False
    )
```

```python
import jax
import jax.numpy as jnp
from jax import lax
from jax.experimental import pallas as pl
from jax.experimental.pallas import tpu as pltpu
from jax.sharding import PartitionSpec as P

MESH = pl.DeviceIdType.MESH
BF = jnp.bfloat16
F32 = jnp.float32
UNITS = 8
BEFORE = (0, 4)
EARLY_Z = (0, 4)
ORDER = (
    "m04", "f15", "m15", "f26", "f37", "m26", "m37", "r15",
    "r26", "z04", "r37", "e1", "e5", "e2", "e6", "e0",
    "e4", "e3", "e7",
)


def kernel(
    snap_ref, steer_ref, comb_ref, list_ref, out_ref,
    snap, steer, order_row, prod, p_send, p_all, lhs, w_all, sel, part, rrecv, tsum, zrecv, zfirst, zsum, rlast, acc,
    load_sem, wload_sem, p_rs, w_rs, r_rs, z_rs, sent, ring_sem,
):
    grp = lax.axis_index("grp")
    sub = lax.axis_index("sub")
    zl, core = grp // 2, grp % 2
    x, zh, y = sub // 16, (sub // 4) % 4, sub % 4
    z = zh * 2 + zl
    other = 1 - core
    gat, red = (x, y), (y, x)
    me = (x * 2 + core, y * 2 + core)

    def dev_g(o, d, c2):
        if o == 0:
            return (zl * 2 + c2, ((x + d) % 4) * 16 + zh * 4 + y)
        return (zl * 2 + c2, x * 16 + zh * 4 + (y + d) % 4)

    def dev_r(o, d):
        return dev_g(1 - o, d, core)

    def dev_z(z2):
        return ((z2 % 2) * 2 + core, x * 16 + (z2 // 2) * 4 + y)

    def zrow(z2):
        return (z2 % 2) * 4 + z2 // 2

    wloads = []
    for u in range(UNITS):
        c = pltpu.make_async_copy(
            comb_ref.at[:, :, pl.ds(u * 128, 128)], w_all.at[u, me[u // 4]], wload_sem.at[u]
        )
        wloads.append(c)
    loads = [
        pltpu.make_async_copy(steer_ref, steer, load_sem.at[0]),
        pltpu.make_async_copy(snap_ref, snap, load_sem.at[1]),
        pltpu.make_async_copy(list_ref, order_row, load_sem.at[2]),
    ]
    for c in [wloads[k] for k in (0, 4, 1, 5)] + loads + [wloads[k] for k in (2, 6, 3, 7)]:
        c.start()

    barrier = pltpu.get_barrier_semaphore()
    peers = [dev_g(o, d, c2) for o in range(2) for d in range(1, 4) for c2 in (core, other)]
    peers += [dev_g(0, 0, other)]
    peers += [dev_z((z + dz) % 8) for dz in (1, 7)]
    for p in peers:
        pl.semaphore_signal(barrier, inc=1, device_id=p, device_id_type=MESH)

    def send(kind, src, dst, rs, dev):
        pltpu.make_async_remote_copy(
            src_ref=src, dst_ref=dst, send_sem=sent.at[kind], recv_sem=rs, device_id=dev,
            device_id_type=MESH,
        ).start()

    def arrived(ref, rs):
        pltpu.make_async_copy(ref, ref, rs).wait()

    def ring_signal(k, hop):
        for j, d in enumerate((hop, 8 - hop)):
            pl.semaphore_signal(
                ring_sem.at[k, j], inc=1, device_id=dev_z((z + d) % 8), device_id_type=MESH
            )

    def ring_wait(k):
        for j in range(2):
            pl.semaphore_wait(ring_sem.at[k, j], 1)

    def w_own(u):
        o = u // 4
        wloads[u].wait()
        mine = w_all.at[u, me[o]]
        for d in (1, 3, 2):
            send(0, mine, mine, w_rs.at[u, 0], dev_g(o, d, core))
        send(0, mine, mine, w_rs.at[u, 1], dev_g(o, 0, other))

    def w_forward(u):
        o = u // 4
        got = [w_all.at[u, ((gat[o] + 4 - d) % 4) * 2 + core] for d in (1, 3, 2)]
        arrived(w_all.at[u, pl.ds(0, 3)], w_rs.at[u, 0])
        for a in got:
            send(0, a, a, w_rs.at[u, 1], dev_g(o, 0, other))

    order = [(2, 0), (2, 1), (1, 0), (3, 0), (1, 1), (3, 1), (0, 1)]

    def first_section():
        for c in loads:
            c.wait()
        s_re, s_im = steer[0], steer[1]
        weights = jnp.concatenate([s_re, s_im, -s_im, s_re], axis=0)
        for half in range(2):
            for c2 in range(2):
                for x2 in range(4):
                    slot = half * 8 + c2 * 4 + x2
                    rows = snap[slot * 256 : slot * 256 + 256, :]
                    both = lax.dot_general(
                        rows, weights, (((1,), (1,)), ((), ())), preferred_element_type=F32
                    )
                    prod[slot, 0] = both[:, :128]
                    prod[slot, 1] = both[:, 128:]
                    val = (
                        prod[slot, 0, pl.ds(0, 128, stride=2)]
                        + prod[slot, 1, pl.ds(1, 128, stride=2)]
                    )
                    for q in range(4):
                        got = jnp.concatenate(
                            [val[h * 32 + q * 8 : h * 32 + q * 8 + 8] for h in range(4)], axis=0
                        ).astype(BF)
                        p_send[0, x2 * 2 + c2, q, half * 32 : half * 32 + 32, :] = got
                        p_send[1, q * 2 + c2, x2, half * 32 : half * 32 + 32, :] = got

    def p_sends():
        for d, dc in order:
            for o in range(2):
                c2 = core if dc == 0 else other
                dest = ((gat[o] + d) % 4) * 2 + c2
                send(1, p_send.at[o, dest], p_all.at[o, me[o]], p_rs.at[o, d], dev_g(o, d, c2))

    def build_lhs(o, d):
        sign = jnp.where(lax.broadcasted_iota(jnp.int32, (256, 128), 1) < 64, 1.0, -1.0).astype(BF)
        base = ((gat[o] + 4 - d) % 4) * 2
        if d:
            arrived(p_all.at[o, pl.ds(base, 2)], p_rs.at[o, d])
        else:
            arrived(p_all.at[o, base + other], p_rs.at[o, d])
        for dc in range(2):
            src = base + (core if dc == 0 else other)
            val = p_all[o, src] if d or dc else p_send[o, src]
            val = val.reshape(256, 128)
            lhs[o, src, 0:256] = val * sign
            lhs[o, src, 256:512] = jnp.concatenate([val[:, 64:], val[:, :64]], axis=1)

    def multiply(units):
        for u in units:
            arrived(w_all.at[u, pl.ds(0, 4)], w_rs.at[u, 1])
        for o in range(2):
            mine = [u for u in units if u // 4 == o]
            left = jnp.concatenate([lhs[o, k] for k in range(8)], axis=1)
            right = jnp.concatenate([w_all[u].reshape(1024, 128) for u in mine], axis=1)
            val = jnp.dot(left, right, preferred_element_type=F32)
            for n, u in enumerate(mine):
                got = val[:, n * 128 : n * 128 + 128]
                got = jnp.concatenate([got[:256].reshape(32, 8, 128), got[256:].reshape(32, 8, 128)], axis=1)
                part[u] = got.astype(BF).reshape(4, 8, 16, 128)
        for u in units:
            if u in EARLY_Z:
                for dz in (4, 3, 5, 2, 6, 1, 7):
                    z2 = (z + dz) % 8
                    send(4, part.at[u, :, zrow(z2)], zfirst.at[EARLY_Z.index(u), dz], z_rs.at[u], dev_z(z2))
            else:
                o = u // 4
                for d in (2, 1, 3):
                    send(2, part.at[u, (red[o] + d) % 4], rrecv.at[u, d], r_rs.at[u], dev_r(o, d))

    def r_sum(u):
        arrived(rrecv.at[u, pl.ds(1, 3)], r_rs.at[u])
        total = part[u, red[u // 4]].astype(F32)
        for d in (1, 3, 2):
            total = total + rrecv[u, d].astype(F32)
        tsum[u] = total.astype(BF)
        for dz in (4, 3, 5, 2, 6, 1, 7):
            z2 = (z + dz) % 8
            send(3, tsum.at[u, zrow(z2)], zrecv.at[u, dz], z_rs.at[u], dev_z(z2))

    def z_sum(u):
        n, o = EARLY_Z.index(u), u // 4
        arrived(zfirst.at[n, pl.ds(1, 7)], z_rs.at[u])
        total = part[u, :, zrow(z)].astype(F32)
        for dz in range(1, 8):
            total = total + zfirst[n, dz].astype(F32)
        zsum[n] = total.astype(BF)
        for d in (2, 1, 3):
            send(5, zsum.at[n, (red[o] + d) % 4], rlast.at[n, d], r_rs.at[u], dev_r(o, d))

    def last_sum(u):
        if u in EARLY_Z:
            n = EARLY_Z.index(u)
            arrived(rlast.at[n, pl.ds(1, 3)], r_rs.at[u])
            total = zsum[n, red[u // 4]].astype(F32)
            for d in range(1, 4):
                total = total + rlast[n, d].astype(F32)
        else:
            arrived(zrecv.at[u, pl.ds(1, 7)], z_rs.at[u])
            total = tsum[u, zrow(z)].astype(F32)
            for dz in range(1, 8):
                total = total + zrecv[u, dz].astype(F32)
        return jnp.dot(
            total.astype(BF), sel[pl.ds(u * 128, 128)], preferred_element_type=F32
        )

    scope = jax.named_scope
    with scope("barrier"):
        pl.semaphore_wait(barrier, len(peers))
    with scope("start"):
        ring_signal(0, 1)
        for u in BEFORE:
            w_own(u)
    with scope("first"):
        first_section()
    with scope("psend"):
        p_sends()
    with scope("w_own"):
        for u in (0, 4, 1, 5, 2, 6, 3, 7):
            if u not in BEFORE:
                w_own(u)
    with scope("sel"):
        for k in range(UNITS // 2):
            rows = lax.broadcasted_iota(jnp.int32, (256, 1024), 0) + k * 256
            sel[pl.ds(k * 256, 256)] = jnp.where(rows == order_row[...], 1.0, 0.0).astype(BF)
    with scope("ring"):
        ring_wait(0)
        ring_signal(1, 2)
    with scope("w_forward_0"):
        for u in BEFORE:
            w_forward(u)
    with scope("lhs"):
        for d in (0, 2, 1, 3):
            for o in range(2):
                build_lhs(o, d)
    with scope("ringwait"):
        ring_wait(1)
    done = 0
    for op in ORDER:
        units = [int(k) for k in op[1:]]
        with scope(op):
            if op[0] == "m":
                multiply(units)
            for u in units:
                if op[0] == "f":
                    w_forward(u)
                elif op[0] == "r":
                    r_sum(u)
                elif op[0] == "z":
                    z_sum(u)
                elif op[0] == "e":
                    val = last_sum(u)
                    done += 1
                    if done == 1:
                        acc[...] = val
                    elif done < UNITS:
                        acc[...] += val
                    else:
                        out_ref[...] = (acc[...] + val).astype(BF)
    with scope("sends"):
        rest = UNITS - len(EARLY_Z)
        arrived(w_all.at[:, pl.ds(0, 7)], sent.at[0])
        arrived(p_all.at[:, pl.ds(0, 7)], sent.at[1])
        arrived(rrecv.at[pl.ds(0, rest), pl.ds(0, 3)], sent.at[2])
        arrived(zrecv.at[pl.ds(0, rest), pl.ds(0, 7)], sent.at[3])
        if EARLY_Z:
            arrived(zfirst.at[:, pl.ds(0, 7)], sent.at[4])
            arrived(rlast.at[:, pl.ds(0, 3)], sent.at[5])


def solution(mesh):
    def step(snapshots, steering, combining, beam_list):
        snaps, _, _, elements = snapshots.shape
        partial = steering.shape[3]
        beams = combining.shape[3]
        dma = pltpu.SemaphoreType.DMA
        out = pl.pallas_call(
            kernel,
            out_shape=pltpu.VMEM((16, beams), BF),
            in_specs=[
                pl.BlockSpec(memory_space=pl.ANY),
                pl.BlockSpec(memory_space=pl.ANY),
                pl.BlockSpec(memory_space=pl.ANY),
                pl.BlockSpec(memory_space=pl.ANY),
            ],
            out_specs=pl.BlockSpec(memory_space=pltpu.VMEM),
            scratch_shapes=[
                pltpu.VMEM((2 * snaps, elements), BF),
                pltpu.VMEM((2, partial, elements), BF),
                pltpu.VMEM((1, beams), jnp.int32),
                pltpu.VMEM((16, 2, 256, 128), F32),
                pltpu.VMEM((2, 8, 4, 64, 128), BF),
                pltpu.VMEM((2, 8, 4, 64, 128), BF),
                pltpu.VMEM((2, 8, 512, 128), BF),
                pltpu.VMEM((UNITS, 8, 2, 64, 128), BF),
                pltpu.VMEM((beams, beams), BF),
                pltpu.VMEM((UNITS, 4, 8, 16, 128), BF),
                pltpu.VMEM((UNITS, 4, 8, 16, 128), BF),
                pltpu.VMEM((UNITS, 8, 16, 128), BF),
                pltpu.VMEM((UNITS, 8, 16, 128), BF),
                pltpu.VMEM((max(1, len(EARLY_Z)), 8, 4, 16, 128), BF),
                pltpu.VMEM((max(1, len(EARLY_Z)), 4, 16, 128), BF),
                pltpu.VMEM((max(1, len(EARLY_Z)), 4, 16, 128), BF),
                pltpu.VMEM((16, beams), F32),
                dma((3,)),
                dma((UNITS,)),
                dma((2, 4)),
                dma((UNITS, 2)),
                dma((UNITS,)),
                dma((UNITS,)),
                dma((6,)),
                pltpu.SemaphoreType.REGULAR((2, 2)),
            ],
            compiler_params=pltpu.CompilerParams(collective_id=0, has_side_effects=True),
        )(
            snapshots[:, :, 0, :].reshape(2 * snaps, elements),
            jnp.swapaxes(steering[0], 1, 2),
            combining[0],
            beam_list.reshape(1, beams),
        )
        return out.reshape(2, 8, beams)

    placed = (
        P(None, None, ("grp", "sub"), None),
        P(("grp", "sub"), None, None, None),
        P(("grp", "sub"), None, None, None),
        P(),
    )
    return jax.shard_map(
        step, mesh=mesh, in_specs=placed, out_specs=P(None, ("grp", "sub"), None), check_vma=False
    )
```

```python
import jax
import jax.numpy as jnp
from jax import lax
from jax.experimental import pallas as pl
from jax.experimental.pallas import tpu as pltpu
from jax.sharding import PartitionSpec as P

MESH = pl.DeviceIdType.MESH
BF = jnp.bfloat16
F32 = jnp.float32
UNITS = 8
BEFORE = (0, 4)
EARLY_Z = (0, 4)
ORDER = (
    "m04", "f15", "m15", "f26", "f37", "m26", "m37", "r15",
    "r26", "z04", "r37", "e1", "e5", "e2", "e6", "e0",
    "e4", "e3", "e7",
)


def kernel(
    snap_ref, steer_ref, comb_ref, list_ref, out_ref,
    snap, steer, order_row, prod, p_send, p_all, lhs, w_all, sel, part, rrecv, tsum, zrecv, zfirst, zsum, rlast, acc,
    load_sem, wload_sem, p_rs, w_rs, r_rs, z_rs, sent, ring_sem,
):
    grp = lax.axis_index("grp")
    sub = lax.axis_index("sub")
    zl, core = grp // 2, grp % 2
    x, zh, y = sub // 16, (sub // 4) % 4, sub % 4
    z = zh * 2 + zl
    other = 1 - core
    gat, red = (x, y), (y, x)
    me = (x * 2 + core, y * 2 + core)

    def dev_g(o, d, c2):
        if o == 0:
            return (zl * 2 + c2, ((x + d) % 4) * 16 + zh * 4 + y)
        return (zl * 2 + c2, x * 16 + zh * 4 + (y + d) % 4)

    def dev_r(o, d):
        return dev_g(1 - o, d, core)

    def dev_z(z2):
        return ((z2 % 2) * 2 + core, x * 16 + (z2 // 2) * 4 + y)

    def zrow(z2):
        return (z2 % 2) * 4 + z2 // 2

    wloads = []
    for u in range(UNITS):
        c = pltpu.make_async_copy(
            comb_ref.at[:, :, pl.ds(u * 128, 128)], w_all.at[u, me[u // 4]], wload_sem.at[int(u not in BEFORE)]
        )
        wloads.append(c)
    loads = [
        pltpu.make_async_copy(steer_ref, steer, load_sem.at[0]),
        pltpu.make_async_copy(snap_ref, snap, load_sem.at[1]),
        pltpu.make_async_copy(list_ref, order_row, load_sem.at[2]),
    ]
    for c in [wloads[k] for k in (0, 4, 1, 5)] + loads + [wloads[k] for k in (2, 6, 3, 7)]:
        c.start()

    barrier = pltpu.get_barrier_semaphore()
    peers = [dev_g(o, d, c2) for o in range(2) for d in range(1, 4) for c2 in (core, other)]
    peers += [dev_g(0, 0, other)]
    peers += [dev_z((z + dz) % 8) for dz in (1, 7)]
    for p in peers:
        pl.semaphore_signal(barrier, inc=1, device_id=p, device_id_type=MESH)

    def send(kind, src, dst, rs, dev):
        pltpu.make_async_remote_copy(
            src_ref=src, dst_ref=dst, send_sem=sent.at[kind], recv_sem=rs, device_id=dev,
            device_id_type=MESH,
        ).start()

    def arrived(ref, rs):
        pltpu.make_async_copy(ref, ref, rs).wait()

    def ring_signal(k, hop):
        for j, d in enumerate((hop, 8 - hop)):
            pl.semaphore_signal(
                ring_sem.at[k, j], inc=1, device_id=dev_z((z + d) % 8), device_id_type=MESH
            )

    def ring_wait(k):
        for j in range(2):
            pl.semaphore_wait(ring_sem.at[k, j], 1)

    def w_own(u):
        o = u // 4
        mine = w_all.at[u, me[o]]
        for d in (1, 3, 2):
            send(0, mine, mine, w_rs.at[u, 0], dev_g(o, d, core))
        send(0, mine, mine, w_rs.at[u, 1], dev_g(o, 0, other))

    def w_forward(u):
        o = u // 4
        got = [w_all.at[u, ((gat[o] + 4 - d) % 4) * 2 + core] for d in (1, 3, 2)]
        arrived(w_all.at[u, pl.ds(0, 3)], w_rs.at[u, 0])
        for a in got:
            send(0, a, a, w_rs.at[u, 1], dev_g(o, 0, other))

    order = [(2, 0), (2, 1), (1, 0), (3, 0), (1, 1), (3, 1), (0, 1)]

    def first_section():
        for c in loads:
            c.wait()
        s_re, s_im = steer[0], steer[1]
        weights = jnp.concatenate([s_re, s_im, -s_im, s_re], axis=0)
        for half in range(2):
            for c2 in range(2):
                for x2 in range(4):
                    slot = half * 8 + c2 * 4 + x2
                    rows = snap[slot * 256 : slot * 256 + 256, :]
                    both = lax.dot_general(
                        rows, weights, (((1,), (1,)), ((), ())), preferred_element_type=F32
                    )
                    prod[slot, 0] = both[:, :128]
                    prod[slot, 1] = both[:, 128:]
                    val = (
                        prod[slot, 0, pl.ds(0, 128, stride=2)]
                        + prod[slot, 1, pl.ds(1, 128, stride=2)]
                    )
                    for q in range(4):
                        got = jnp.concatenate(
                            [val[h * 32 + q * 8 : h * 32 + q * 8 + 8] for h in range(4)], axis=0
                        ).astype(BF)
                        p_send[0, x2 * 2 + c2, q, half * 32 : half * 32 + 32, :] = got
                        p_send[1, q * 2 + c2, x2, half * 32 : half * 32 + 32, :] = got

    def p_sends():
        for d, dc in order:
            for o in range(2):
                c2 = core if dc == 0 else other
                dest = ((gat[o] + d) % 4) * 2 + c2
                send(1, p_send.at[o, dest], p_all.at[o, me[o]], p_rs.at[o, d], dev_g(o, d, c2))

    def build_lhs(o, d):
        sign = jnp.where(lax.broadcasted_iota(jnp.int32, (256, 128), 1) < 64, 1.0, -1.0).astype(BF)
        base = ((gat[o] + 4 - d) % 4) * 2
        if d:
            arrived(p_all.at[o, pl.ds(base, 2)], p_rs.at[o, d])
        else:
            arrived(p_all.at[o, base + other], p_rs.at[o, d])
        for dc in range(2):
            src = base + (core if dc == 0 else other)
            val = p_all[o, src] if d or dc else p_send[o, src]
            val = val.reshape(256, 128)
            lhs[o, src, 0:256] = val * sign
            lhs[o, src, 256:512] = jnp.concatenate([val[:, 64:], val[:, :64]], axis=1)

    def multiply(units):
        for u in units:
            arrived(w_all.at[u, pl.ds(0, 4)], w_rs.at[u, 1])
        for o in range(2):
            mine = [u for u in units if u // 4 == o]
            left = jnp.concatenate([lhs[o, k] for k in range(8)], axis=1)
            right = jnp.concatenate([w_all[u].reshape(1024, 128) for u in mine], axis=1)
            val = jnp.dot(left, right, preferred_element_type=F32)
            for n, u in enumerate(mine):
                got = val[:, n * 128 : n * 128 + 128]
                got = jnp.concatenate([got[:256].reshape(32, 8, 128), got[256:].reshape(32, 8, 128)], axis=1)
                part[u] = got.astype(BF).reshape(4, 8, 16, 128)
        for u in units:
            if u in EARLY_Z:
                for dz in (4, 3, 5, 2, 6, 1, 7):
                    z2 = (z + dz) % 8
                    send(4, part.at[u, :, zrow(z2)], zfirst.at[EARLY_Z.index(u), dz], z_rs.at[u], dev_z(z2))
            else:
                o = u // 4
                for d in (2, 1, 3):
                    send(2, part.at[u, (red[o] + d) % 4], rrecv.at[u, d], r_rs.at[u], dev_r(o, d))

    def r_sum(u):
        arrived(rrecv.at[u, pl.ds(1, 3)], r_rs.at[u])
        total = part[u, red[u // 4]].astype(F32)
        for d in (1, 3, 2):
            total = total + rrecv[u, d].astype(F32)
        tsum[u] = total.astype(BF)
        for dz in (4, 3, 5, 2, 6, 1, 7):
            z2 = (z + dz) % 8
            send(3, tsum.at[u, zrow(z2)], zrecv.at[u, dz], z_rs.at[u], dev_z(z2))

    def z_sum(u):
        n, o = EARLY_Z.index(u), u // 4
        arrived(zfirst.at[n, pl.ds(1, 7)], z_rs.at[u])
        total = part[u, :, zrow(z)].astype(F32)
        for dz in range(1, 8):
            total = total + zfirst[n, dz].astype(F32)
        zsum[n] = total.astype(BF)
        for d in (2, 1, 3):
            send(5, zsum.at[n, (red[o] + d) % 4], rlast.at[n, d], r_rs.at[u], dev_r(o, d))

    def last_sum(u):
        if u in EARLY_Z:
            n = EARLY_Z.index(u)
            arrived(rlast.at[n, pl.ds(1, 3)], r_rs.at[u])
            total = zsum[n, red[u // 4]].astype(F32)
            for d in range(1, 4):
                total = total + rlast[n, d].astype(F32)
        else:
            arrived(zrecv.at[u, pl.ds(1, 7)], z_rs.at[u])
            total = tsum[u, zrow(z)].astype(F32)
            for dz in range(1, 8):
                total = total + zrecv[u, dz].astype(F32)
        return jnp.dot(
            total.astype(BF), sel[pl.ds(u * 128, 128)], preferred_element_type=F32
        )

    scope = jax.named_scope
    with scope("barrier"):
        pl.semaphore_wait(barrier, len(peers))
    with scope("start"):
        ring_signal(0, 1)
        arrived(w_all.at[pl.ds(0, len(BEFORE)), 0], wload_sem.at[0])
        for u in BEFORE:
            w_own(u)
    with scope("first"):
        first_section()
    with scope("psend"):
        p_sends()
    with scope("w_own"):
        arrived(w_all.at[pl.ds(0, UNITS - len(BEFORE)), 0], wload_sem.at[1])
        for u in (0, 4, 1, 5, 2, 6, 3, 7):
            if u not in BEFORE:
                w_own(u)
    with scope("sel"):
        for k in range(UNITS // 2):
            rows = lax.broadcasted_iota(jnp.int32, (256, 1024), 0) + k * 256
            sel[pl.ds(k * 256, 256)] = jnp.where(rows == order_row[...], 1.0, 0.0).astype(BF)
    with scope("ring"):
        ring_wait(0)
        ring_signal(1, 2)
    with scope("w_forward_0"):
        for u in BEFORE:
            w_forward(u)
    with scope("lhs"):
        for d in (0, 2, 1, 3):
            for o in range(2):
                build_lhs(o, d)
    with scope("ringwait"):
        ring_wait(1)
    done = 0
    for op in ORDER:
        units = [int(k) for k in op[1:]]
        with scope(op):
            if op[0] == "m":
                multiply(units)
            for u in units:
                if op[0] == "f":
                    w_forward(u)
                elif op[0] == "r":
                    r_sum(u)
                elif op[0] == "z":
                    z_sum(u)
                elif op[0] == "e":
                    val = last_sum(u)
                    done += 1
                    if done == 1:
                        acc[...] = val
                    elif done < UNITS:
                        acc[...] += val
                    else:
                        out_ref[...] = (acc[...] + val).astype(BF)
    with scope("sends"):
        rest = UNITS - len(EARLY_Z)
        arrived(w_all.at[:, pl.ds(0, 7)], sent.at[0])
        arrived(p_all.at[:, pl.ds(0, 7)], sent.at[1])
        arrived(rrecv.at[pl.ds(0, rest), pl.ds(0, 3)], sent.at[2])
        arrived(zrecv.at[pl.ds(0, rest), pl.ds(0, 7)], sent.at[3])
        if EARLY_Z:
            arrived(zfirst.at[:, pl.ds(0, 7)], sent.at[4])
            arrived(rlast.at[:, pl.ds(0, 3)], sent.at[5])


def solution(mesh):
    def step(snapshots, steering, combining, beam_list):
        snaps, _, _, elements = snapshots.shape
        partial = steering.shape[3]
        beams = combining.shape[3]
        dma = pltpu.SemaphoreType.DMA
        out = pl.pallas_call(
            kernel,
            out_shape=pltpu.VMEM((16, beams), BF),
            in_specs=[
                pl.BlockSpec(memory_space=pl.ANY),
                pl.BlockSpec(memory_space=pl.ANY),
                pl.BlockSpec(memory_space=pl.ANY),
                pl.BlockSpec(memory_space=pl.ANY),
            ],
            out_specs=pl.BlockSpec(memory_space=pltpu.VMEM),
            scratch_shapes=[
                pltpu.VMEM((2 * snaps, elements), BF),
                pltpu.VMEM((2, partial, elements), BF),
                pltpu.VMEM((1, beams), jnp.int32),
                pltpu.VMEM((16, 2, 256, 128), F32),
                pltpu.VMEM((2, 8, 4, 64, 128), BF),
                pltpu.VMEM((2, 8, 4, 64, 128), BF),
                pltpu.VMEM((2, 8, 512, 128), BF),
                pltpu.VMEM((UNITS, 8, 2, 64, 128), BF),
                pltpu.VMEM((beams, beams), BF),
                pltpu.VMEM((UNITS, 4, 8, 16, 128), BF),
                pltpu.VMEM((UNITS, 4, 8, 16, 128), BF),
                pltpu.VMEM((UNITS, 8, 16, 128), BF),
                pltpu.VMEM((UNITS, 8, 16, 128), BF),
                pltpu.VMEM((max(1, len(EARLY_Z)), 8, 4, 16, 128), BF),
                pltpu.VMEM((max(1, len(EARLY_Z)), 4, 16, 128), BF),
                pltpu.VMEM((max(1, len(EARLY_Z)), 4, 16, 128), BF),
                pltpu.VMEM((16, beams), F32),
                dma((3,)),
                dma((2,)),
                dma((2, 4)),
                dma((UNITS, 2)),
                dma((UNITS,)),
                dma((UNITS,)),
                dma((6,)),
                pltpu.SemaphoreType.REGULAR((2, 2)),
            ],
            compiler_params=pltpu.CompilerParams(collective_id=0, has_side_effects=True),
        )(
            snapshots[:, :, 0, :].reshape(2 * snaps, elements),
            jnp.swapaxes(steering[0], 1, 2),
            combining[0],
            beam_list.reshape(1, beams),
        )
        return out.reshape(2, 8, beams)

    placed = (
        P(None, None, ("grp", "sub"), None),
        P(("grp", "sub"), None, None, None),
        P(("grp", "sub"), None, None, None),
        P(),
    )
    return jax.shard_map(
        step, mesh=mesh, in_specs=placed, out_specs=P(None, ("grp", "sub"), None), check_vma=False
    )
```

```python
import jax
import jax.numpy as jnp
from jax import lax
from jax.experimental import pallas as pl
from jax.experimental.pallas import tpu as pltpu
from jax.sharding import PartitionSpec as P

MESH = pl.DeviceIdType.MESH
BF = jnp.bfloat16
F32 = jnp.float32
UNITS = 8
BEFORE = (0, 4)
EARLY_Z = (0, 4)
ORDER = (
    "m04", "f15", "m15", "f26", "f37", "m26", "m37", "r15",
    "z04", "r26", "r37", "e1", "e5", "e0", "e4", "e2",
    "e6", "e3", "e7",
)


def kernel(
    snap_ref, steer_ref, comb_ref, list_ref, out_ref,
    snap, steer, order_row, prod, p_send, p_all, lhs, w_all, sel, part, rrecv, tsum, zrecv, zfirst, zsum, rlast, acc,
    load_sem, wload_sem, p_rs, w_rs, r_rs, z_rs, sent, ring_sem,
):
    grp = lax.axis_index("grp")
    sub = lax.axis_index("sub")
    zl, core = grp // 2, grp % 2
    x, zh, y = sub // 16, (sub // 4) % 4, sub % 4
    z = zh * 2 + zl
    other = 1 - core
    gat, red = (x, y), (y, x)
    me = (x * 2 + core, y * 2 + core)

    def dev_g(o, d, c2):
        if o == 0:
            return (zl * 2 + c2, ((x + d) % 4) * 16 + zh * 4 + y)
        return (zl * 2 + c2, x * 16 + zh * 4 + (y + d) % 4)

    def dev_r(o, d):
        return dev_g(1 - o, d, core)

    def dev_z(z2):
        return ((z2 % 2) * 2 + core, x * 16 + (z2 // 2) * 4 + y)

    def zrow(z2):
        return (z2 % 2) * 4 + z2 // 2

    wloads = []
    for u in range(UNITS):
        c = pltpu.make_async_copy(
            comb_ref.at[:, :, pl.ds(u * 128, 128)], w_all.at[u, me[u // 4]], wload_sem.at[int(u not in BEFORE)]
        )
        wloads.append(c)
    loads = [
        pltpu.make_async_copy(steer_ref, steer, load_sem.at[0]),
        pltpu.make_async_copy(snap_ref, snap, load_sem.at[1]),
        pltpu.make_async_copy(list_ref, order_row, load_sem.at[2]),
    ]
    for c in [wloads[k] for k in (0, 4, 1, 5)] + loads + [wloads[k] for k in (2, 6, 3, 7)]:
        c.start()

    barrier = pltpu.get_barrier_semaphore()
    peers = [dev_g(o, d, c2) for o in range(2) for d in range(1, 4) for c2 in (core, other)]
    peers += [dev_g(0, 0, other)]
    peers += [dev_z((z + dz) % 8) for dz in (1, 7)]
    for p in peers:
        pl.semaphore_signal(barrier, inc=1, device_id=p, device_id_type=MESH)

    def send(kind, src, dst, rs, dev):
        pltpu.make_async_remote_copy(
            src_ref=src, dst_ref=dst, send_sem=sent.at[kind], recv_sem=rs, device_id=dev,
            device_id_type=MESH,
        ).start()

    def arrived(ref, rs):
        pltpu.make_async_copy(ref, ref, rs).wait()

    def ring_signal(k, hop):
        for j, d in enumerate((hop, 8 - hop)):
            pl.semaphore_signal(
                ring_sem.at[k, j], inc=1, device_id=dev_z((z + d) % 8), device_id_type=MESH
            )

    def ring_wait(k):
        for j in range(2):
            pl.semaphore_wait(ring_sem.at[k, j], 1)

    def w_own(u):
        o = u // 4
        mine = w_all.at[u, me[o]]
        for d in (1, 3, 2):
            send(0, mine, mine, w_rs.at[u, 0], dev_g(o, d, core))
        send(0, mine, mine, w_rs.at[u, 1], dev_g(o, 0, other))

    def w_forward(u):
        o = u // 4
        got = [w_all.at[u, ((gat[o] + 4 - d) % 4) * 2 + core] for d in (1, 3, 2)]
        arrived(w_all.at[u, pl.ds(0, 3)], w_rs.at[u, 0])
        for a in got:
            send(0, a, a, w_rs.at[u, 1], dev_g(o, 0, other))

    order = [(2, 0), (2, 1), (1, 0), (3, 0), (1, 1), (3, 1), (0, 1)]

    def first_section():
        for c in loads:
            c.wait()
        s_re, s_im = steer[0], steer[1]
        weights = jnp.concatenate([s_re, s_im, -s_im, s_re], axis=0)
        for half in range(2):
            for c2 in range(2):
                for x2 in range(4):
                    slot = half * 8 + c2 * 4 + x2
                    rows = snap[slot * 256 : slot * 256 + 256, :]
                    both = lax.dot_general(
                        rows, weights, (((1,), (1,)), ((), ())), preferred_element_type=F32
                    )
                    prod[slot, 0] = both[:, :128]
                    prod[slot, 1] = both[:, 128:]
                    val = (
                        prod[slot, 0, pl.ds(0, 128, stride=2)]
                        + prod[slot, 1, pl.ds(1, 128, stride=2)]
                    )
                    for q in range(4):
                        got = jnp.concatenate(
                            [val[h * 32 + q * 8 : h * 32 + q * 8 + 8] for h in range(4)], axis=0
                        ).astype(BF)
                        p_send[0, x2 * 2 + c2, q, half * 32 : half * 32 + 32, :] = got
                        p_send[1, q * 2 + c2, x2, half * 32 : half * 32 + 32, :] = got

    def p_sends():
        for d, dc in order:
            for o in range(2):
                c2 = core if dc == 0 else other
                dest = ((gat[o] + d) % 4) * 2 + c2
                send(1, p_send.at[o, dest], p_all.at[o, me[o]], p_rs.at[o, d], dev_g(o, d, c2))

    def build_lhs(o, d):
        sign = jnp.where(lax.broadcasted_iota(jnp.int32, (256, 128), 1) < 64, 1.0, -1.0).astype(BF)
        base = ((gat[o] + 4 - d) % 4) * 2
        if d:
            arrived(p_all.at[o, pl.ds(base, 2)], p_rs.at[o, d])
        else:
            arrived(p_all.at[o, base + other], p_rs.at[o, d])
        for dc in range(2):
            src = base + (core if dc == 0 else other)
            val = p_all[o, src] if d or dc else p_send[o, src]
            val = val.reshape(256, 128)
            lhs[o, src, 0:256] = val * sign
            lhs[o, src, 256:512] = jnp.concatenate([val[:, 64:], val[:, :64]], axis=1)

    def multiply(units):
        for u in units:
            arrived(w_all.at[u, pl.ds(0, 4)], w_rs.at[u, 1])
        for o in range(2):
            mine = [u for u in units if u // 4 == o]
            left = jnp.concatenate([lhs[o, k] for k in range(8)], axis=1)
            right = jnp.concatenate([w_all[u].reshape(1024, 128) for u in mine], axis=1)
            val = jnp.dot(left, right, preferred_element_type=F32)
            for n, u in enumerate(mine):
                got = val[:, n * 128 : n * 128 + 128]
                got = jnp.concatenate([got[:256].reshape(32, 8, 128), got[256:].reshape(32, 8, 128)], axis=1)
                part[u] = got.astype(BF).reshape(4, 8, 16, 128)
        for u in units:
            if u in EARLY_Z:
                for dz in (4, 3, 5, 2, 6, 1, 7):
                    z2 = (z + dz) % 8
                    send(4, part.at[u, :, zrow(z2)], zfirst.at[EARLY_Z.index(u), dz], z_rs.at[u], dev_z(z2))
            else:
                o = u // 4
                for d in (2, 1, 3):
                    send(2, part.at[u, (red[o] + d) % 4], rrecv.at[u, d], r_rs.at[u], dev_r(o, d))

    def r_sum(u):
        arrived(rrecv.at[u, pl.ds(1, 3)], r_rs.at[u])
        total = part[u, red[u // 4]].astype(F32)
        for d in (1, 3, 2):
            total = total + rrecv[u, d].astype(F32)
        tsum[u] = total.astype(BF)
        for dz in (4, 3, 5, 2, 6, 1, 7):
            z2 = (z + dz) % 8
            send(3, tsum.at[u, zrow(z2)], zrecv.at[u, dz], z_rs.at[u], dev_z(z2))

    def z_sum(u):
        n, o = EARLY_Z.index(u), u // 4
        arrived(zfirst.at[n, pl.ds(1, 7)], z_rs.at[u])
        total = part[u, :, zrow(z)].astype(F32)
        for dz in range(1, 8):
            total = total + zfirst[n, dz].astype(F32)
        zsum[n] = total.astype(BF)
        for d in (2, 1, 3):
            send(5, zsum.at[n, (red[o] + d) % 4], rlast.at[n, d], r_rs.at[u], dev_r(o, d))

    def last_sum(u):
        if u in EARLY_Z:
            n = EARLY_Z.index(u)
            arrived(rlast.at[n, pl.ds(1, 3)], r_rs.at[u])
            total = zsum[n, red[u // 4]].astype(F32)
            for d in range(1, 4):
                total = total + rlast[n, d].astype(F32)
        else:
            arrived(zrecv.at[u, pl.ds(1, 7)], z_rs.at[u])
            total = tsum[u, zrow(z)].astype(F32)
            for dz in range(1, 8):
                total = total + zrecv[u, dz].astype(F32)
        return jnp.dot(
            total.astype(BF), sel[pl.ds(u * 128, 128)], preferred_element_type=F32
        )

    scope = jax.named_scope
    with scope("barrier"):
        pl.semaphore_wait(barrier, len(peers))
    with scope("start"):
        ring_signal(0, 1)
        arrived(w_all.at[pl.ds(0, len(BEFORE)), 0], wload_sem.at[0])
        for u in BEFORE:
            w_own(u)
    with scope("first"):
        first_section()
    with scope("psend"):
        p_sends()
    with scope("w_own"):
        arrived(w_all.at[pl.ds(0, UNITS - len(BEFORE)), 0], wload_sem.at[1])
        for u in (0, 4, 1, 5, 2, 6, 3, 7):
            if u not in BEFORE:
                w_own(u)
    with scope("sel"):
        for k in range(UNITS // 2):
            rows = lax.broadcasted_iota(jnp.int32, (256, 1024), 0) + k * 256
            sel[pl.ds(k * 256, 256)] = jnp.where(rows == order_row[...], 1.0, 0.0).astype(BF)
    with scope("ring"):
        ring_wait(0)
        ring_signal(1, 2)
    with scope("w_forward_0"):
        for u in BEFORE:
            w_forward(u)
    with scope("lhs"):
        for d in (0, 2, 1, 3):
            for o in range(2):
                build_lhs(o, d)
    with scope("ringwait"):
        ring_wait(1)
    done = 0
    for op in ORDER:
        units = [int(k) for k in op[1:]]
        with scope(op):
            if op[0] == "m":
                multiply(units)
            for u in units:
                if op[0] == "f":
                    w_forward(u)
                elif op[0] == "r":
                    r_sum(u)
                elif op[0] == "z":
                    z_sum(u)
                elif op[0] == "e":
                    val = last_sum(u)
                    done += 1
                    if done == 1:
                        acc[...] = val
                    elif done < UNITS:
                        acc[...] += val
                    else:
                        out_ref[...] = (acc[...] + val).astype(BF)
    with scope("sends"):
        rest = UNITS - len(EARLY_Z)
        arrived(w_all.at[:, pl.ds(0, 7)], sent.at[0])
        arrived(p_all.at[:, pl.ds(0, 7)], sent.at[1])
        arrived(rrecv.at[pl.ds(0, rest), pl.ds(0, 3)], sent.at[2])
        arrived(zrecv.at[pl.ds(0, rest), pl.ds(0, 7)], sent.at[3])
        if EARLY_Z:
            arrived(zfirst.at[:, pl.ds(0, 7)], sent.at[4])
            arrived(rlast.at[:, pl.ds(0, 3)], sent.at[5])


def solution(mesh):
    def step(snapshots, steering, combining, beam_list):
        snaps, _, _, elements = snapshots.shape
        partial = steering.shape[3]
        beams = combining.shape[3]
        dma = pltpu.SemaphoreType.DMA
        out = pl.pallas_call(
            kernel,
            out_shape=pltpu.VMEM((16, beams), BF),
            in_specs=[
                pl.BlockSpec(memory_space=pl.ANY),
                pl.BlockSpec(memory_space=pl.ANY),
                pl.BlockSpec(memory_space=pl.ANY),
                pl.BlockSpec(memory_space=pl.ANY),
            ],
            out_specs=pl.BlockSpec(memory_space=pltpu.VMEM),
            scratch_shapes=[
                pltpu.VMEM((2 * snaps, elements), BF),
                pltpu.VMEM((2, partial, elements), BF),
                pltpu.VMEM((1, beams), jnp.int32),
                pltpu.VMEM((16, 2, 256, 128), F32),
                pltpu.VMEM((2, 8, 4, 64, 128), BF),
                pltpu.VMEM((2, 8, 4, 64, 128), BF),
                pltpu.VMEM((2, 8, 512, 128), BF),
                pltpu.VMEM((UNITS, 8, 2, 64, 128), BF),
                pltpu.VMEM((beams, beams), BF),
                pltpu.VMEM((UNITS, 4, 8, 16, 128), BF),
                pltpu.VMEM((UNITS, 4, 8, 16, 128), BF),
                pltpu.VMEM((UNITS, 8, 16, 128), BF),
                pltpu.VMEM((UNITS, 8, 16, 128), BF),
                pltpu.VMEM((max(1, len(EARLY_Z)), 8, 4, 16, 128), BF),
                pltpu.VMEM((max(1, len(EARLY_Z)), 4, 16, 128), BF),
                pltpu.VMEM((max(1, len(EARLY_Z)), 4, 16, 128), BF),
                pltpu.VMEM((16, beams), F32),
                dma((3,)),
                dma((2,)),
                dma((2, 4)),
                dma((UNITS, 2)),
                dma((UNITS,)),
                dma((UNITS,)),
                dma((6,)),
                pltpu.SemaphoreType.REGULAR((2, 2)),
            ],
            compiler_params=pltpu.CompilerParams(collective_id=0, has_side_effects=True),
        )(
            snapshots[:, :, 0, :].reshape(2 * snaps, elements),
            jnp.swapaxes(steering[0], 1, 2),
            combining[0],
            beam_list.reshape(1, beams),
        )
        return out.reshape(2, 8, beams)

    placed = (
        P(None, None, ("grp", "sub"), None),
        P(("grp", "sub"), None, None, None),
        P(("grp", "sub"), None, None, None),
        P(),
    )
    return jax.shard_map(
        step, mesh=mesh, in_specs=placed, out_specs=P(None, ("grp", "sub"), None), check_vma=False
    )
```
